32 devices in a mesh: dp: 1 (over z), ep: 32 (over y, x, core).
Axes of the slice: x: 4, y: 4, z: 1, core: 2. Of those that a mesh axis runs over, the one named last changes fastest.
The devices are a block of a 4x4x8 slice.
Arguments:
- x_rows: bfloat16 [32768, 2048], P(('dp', 'ep'))
- logits: float32 [32768, 256], P(('dp', 'ep'))
- w_in: bfloat16 [256, 2048, 512], P('ep')
- w_out: bfloat16 [256, 512, 2048], P('ep')
Outputs:
- output: bfloat16 [32768, 2048], P(('dp', 'ep'))
All inputs are finite; a program needn't handle non-finite values.
Results may differ from the reference program's by a relative error of at most 0.001.
Values are sent between devices in bfloat16 or wider.
A program may use at most 768 MiB of HBM per device.

```python
import math
import jax
import jax.numpy as jnp
from jax import lax

TOKENS = 32768
D_MODEL = 2048
FF_HIDDEN = 512
EXPERTS = 256
CAPACITY = 256
GROUP_DEV = 32
LOGIT_SHIFT = int(1024 * math.log(EXPERTS))


def draw_logits(route_key):
    sub_keys = jax.random.split(route_key, 5)
    tok_dev = TOKENS // GROUP_DEV
    mean_cnt = 2 * tok_dev // EXPERTS
    quarter = EXPERTS // 4
    exp_order = jax.random.permutation(sub_keys[0], EXPERTS)
    rot_bits = jax.random.randint(sub_keys[1], (GROUP_DEV,), 0, 2)
    tier_vals = jnp.array([2 * mean_cnt, mean_cnt, mean_cnt // 2, mean_cnt // 2], dtype=jnp.int32)
    tier_idx = (jnp.arange(EXPERTS)[None, :] // quarter + rot_bits[:, None]) % 4
    slot_ends = jnp.cumsum(tier_vals[tier_idx], axis=1)
    slot_ids = jnp.arange(2 * tok_dev)
    rank_pos = jnp.sum((slot_ends[:, None, :] <= slot_ids[None, :, None]).astype(jnp.int32), axis=2)
    pick_list = exp_order[rank_pos]
    perm_keys = jax.random.split(sub_keys[2], GROUP_DEV)
    tok_perm = jax.vmap(lambda perm_key: jax.random.permutation(perm_key, tok_dev))(perm_keys)
    first_pick = jnp.take_along_axis(pick_list[:, :tok_dev], tok_perm, axis=1).reshape(TOKENS)
    second_pick = jnp.take_along_axis(pick_list[:, tok_dev:], tok_perm, axis=1).reshape(TOKENS)
    expert_ids = jnp.arange(EXPERTS)
    chosen = (expert_ids[None, :] == first_pick[:, None]) | (expert_ids[None, :] == second_pick[:, None])
    base_val = jax.random.randint(sub_keys[3], (TOKENS, EXPERTS), 0, 2048)
    pick_val = jax.random.randint(sub_keys[4], (TOKENS, EXPERTS), 1024, 3072) + LOGIT_SHIFT
    score_int = jnp.where(chosen, pick_val, base_val) * EXPERTS + expert_ids[None, :]
    return score_int.astype(jnp.float32) / (1024.0 * EXPERTS)


def setup_inputs(seed: int = 0, part: int = 0) -> dict:
    part_key = jax.random.fold_in(jax.random.key(seed), part)
    sub_keys = jax.random.split(part_key, 2)
    w_keys = jax.random.split(jax.random.key(seed + 1), 2)
    x_rows = jax.random.normal(sub_keys[0], (TOKENS, D_MODEL), jnp.float32).astype(jnp.bfloat16)
    logits = draw_logits(sub_keys[1])
    w_in = (jax.random.normal(w_keys[0], (EXPERTS, D_MODEL, FF_HIDDEN), jnp.float32) * D_MODEL ** -0.5).astype(jnp.bfloat16)
    w_out = (jax.random.normal(w_keys[1], (EXPERTS, FF_HIDDEN, D_MODEL), jnp.float32) * (2.0 * FF_HIDDEN ** -0.5)).astype(jnp.bfloat16)
    return {'x_rows': x_rows, 'logits': logits, 'w_in': w_in, 'w_out': w_out}


def reference(x_rows, logits, w_in, w_out):
    gate_probs = jax.nn.softmax(logits, axis=-1)
    top_vals, top_ids = lax.top_k(logits, 2)
    chosen = (logits >= top_vals[:, 1:2]).astype(jnp.int32)
    before = jnp.cumsum(chosen, axis=0) - chosen
    pick_pos = jnp.take_along_axis(before, top_ids, axis=1)
    dest_row = jnp.where(pick_pos < CAPACITY, top_ids * CAPACITY + pick_pos, EXPERTS * CAPACITY)
    tok_ids = jnp.broadcast_to(jnp.arange(TOKENS, dtype=jnp.int32)[:, None], (TOKENS, 2))
    slot_tok = jnp.full((EXPERTS * CAPACITY,), TOKENS, jnp.int32).at[dest_row.reshape(-1)].set(tok_ids.reshape(-1), mode='drop')
    expert_rows = jnp.take(x_rows, slot_tok, axis=0, mode='fill', fill_value=0).reshape(EXPERTS, CAPACITY, D_MODEL)

    def expert_ffn(operands):
        rows_in, w_first, w_second = operands
        hidden = jax.nn.gelu(jnp.dot(rows_in, w_first, preferred_element_type=jnp.float32), approximate=True).astype(jnp.bfloat16)
        return jnp.dot(hidden, w_second, preferred_element_type=jnp.float32).astype(jnp.bfloat16)

    expert_out = lax.map(expert_ffn, (expert_rows, w_in, w_out)).reshape(EXPERTS * CAPACITY, D_MODEL)
    rows_back = jnp.take(expert_out, dest_row, axis=0, mode='fill', fill_value=0)
    pick_gate = jnp.take_along_axis(gate_probs, top_ids, axis=1)
    mix_sum = jnp.sum(pick_gate[:, :, None] * rows_back.astype(jnp.float32), axis=1)
    return (x_rows.astype(jnp.float32) + mix_sum).astype(jnp.bfloat16)
```

```python
import functools

import jax
import jax.numpy as jnp
from jax import lax
from jax.experimental import pallas as pl
from jax.experimental.pallas import tpu as pltpu
from jax.sharding import PartitionSpec as P

CAP_FACTOR = 2
SLOT_FACTOR = 4
CORES = 2
SUB = 16
LANE = 128
VMEM_LIMIT = 62 * 1024 * 1024
BF16 = jnp.bfloat16
F32 = jnp.float32
I32 = jnp.int32


def iota(shape, dim):
    return lax.broadcasted_iota(I32, shape, dim)


def route_kernel(logits_ref, tok_ref, gate_ref, count_ref):
    tokens, experts = logits_ref.shape
    lt = logits_ref[...].T
    ids = iota(lt.shape, 0)
    m1 = jnp.max(lt, axis=0, keepdims=True)
    e1 = jnp.min(jnp.where(lt == m1, ids, experts), axis=0, keepdims=True)
    rest = jnp.where(ids == e1, -jnp.inf, lt)
    m2 = jnp.max(rest, axis=0, keepdims=True)
    e2 = jnp.min(jnp.where(rest == m2, ids, experts), axis=0, keepdims=True)
    total = jnp.sum(jnp.exp(lt - m1), axis=0, keepdims=True)
    hit1 = ids == e1
    hit2 = ids == e2
    chosen = jnp.where(hit1 | hit2, 1.0, 0.0).astype(BF16)
    upper = jnp.where(iota((tokens, tokens), 0) < iota((tokens, tokens), 1), 1.0, 0.0).astype(BF16)
    before = jnp.dot(chosen, upper, preferred_element_type=F32)
    pos1 = jnp.sum(jnp.where(hit1, before, 0.0), axis=0, keepdims=True)
    pos2 = jnp.sum(jnp.where(hit2, before, 0.0), axis=0, keepdims=True)
    tok_ref[0:1, :] = e1
    tok_ref[1:2, :] = e2
    tok_ref[2:3, :] = pos1.astype(I32)
    tok_ref[3:4, :] = pos2.astype(I32)
    gate_ref[0:1, :] = 1.0 / total
    gate_ref[1:2, :] = jnp.exp(m2 - m1) / total
    ones = jnp.ones((8, tokens), BF16)
    count_ref[...] = lax.dot_general(ones, chosen, (((1,), (1,)), ((), ())), preferred_element_type=F32)


def plan_kernel(sizes, capacity, exp_dev, me_ref, counts_ref, tok_ref, gate_ref,
                row_ref, keep_ref, start_ref, cnt_ref, pick_ref):
    devs, experts = counts_ref.shape
    tokens = tok_ref.shape[1]
    exp_chip = CORES * exp_dev
    me = me_ref[0]
    chip = me // CORES
    core = me % CORES
    counts = counts_ref[...]
    lower = jnp.where(iota((devs, devs), 1) < iota((devs, devs), 0), 1.0, 0.0).astype(BF16)
    offs = jnp.dot(lower, counts.astype(BF16), preferred_element_type=F32)
    kept = jnp.minimum(jnp.maximum(capacity - offs, 0.0), counts)
    kept_b = kept.astype(BF16)
    row_e = iota((experts, experts), 0)
    col_e = iota((experts, experts), 1)
    same = (row_e // exp_chip == col_e // exp_chip) & (row_e < col_e)
    start = jnp.dot(kept_b, jnp.where(same, 1.0, 0.0).astype(BF16), preferred_element_type=F32)
    start_b = start.astype(BF16)
    member = jnp.where(iota((experts, LANE), 0) // exp_chip == iota((experts, LANE), 1), 1.0, 0.0).astype(BF16)
    totals = jnp.dot(kept_b, member, preferred_element_type=F32)
    most = jnp.max(jnp.max(totals, axis=0, keepdims=True), axis=1, keepdims=True).astype(I32)
    size = jnp.full((1, 1), sizes[0], I32)
    pick = jnp.zeros((1, 1), I32)
    for small, large in zip(sizes[:-1], sizes[1:]):
        size = jnp.where(most > small, large, size)
        pick = pick + jnp.where(most > small, 1, 0)
    pick_ref[...] = jnp.broadcast_to(pick, pick_ref.shape)

    mine = iota((devs, experts), 0) == me
    my_start = jnp.sum(jnp.where(mine, start, 0.0), axis=0, keepdims=True)
    my_kept = jnp.sum(jnp.where(mine, kept, 0.0), axis=0, keepdims=True)
    look = jnp.concatenate([my_start, my_kept, jnp.zeros((6, experts), F32)], axis=0).astype(BF16)
    ids = iota((experts, tokens), 0)
    lanes = experts // exp_chip
    for k in range(2):
        e = tok_ref[k:k + 1, :]
        pos = tok_ref[2 + k:3 + k, :]
        hit = jnp.where(ids == e, 1.0, 0.0).astype(BF16)
        got = jnp.dot(look, hit, preferred_element_type=F32).astype(I32)
        keep = pos < got[1:2, :]
        row = (e // exp_chip) * size + got[0:1, :] + pos
        row_ref[k:k + 1, :] = jnp.where(keep, row, lanes * size)
        keep_ref[k:k + 1, :] = jnp.where(keep, gate_ref[k:k + 1, :], 0.0)

    srcs = devs // CORES
    pick_src = jnp.where(iota((srcs, devs), 1) == CORES * iota((srcs, devs), 0) + core, 1.0, 0.0).astype(BF16)
    pick_exp = jnp.where(iota((experts, LANE), 0) == chip * exp_chip + iota((experts, LANE), 1), 1.0, 0.0).astype(BF16)
    for src, dst in ((start_b, start_ref), (kept_b, cnt_ref)):
        part = jnp.dot(pick_src, src, preferred_element_type=F32).astype(BF16)
        dst[...] = jnp.dot(part, pick_exp, preferred_element_type=F32).astype(I32)


def send_kernel(size, row_ref, x_ref, out_ref, tok, rows3, stage, sem):
    tokens, d_model = x_ref.shape
    lanes = out_ref.shape[0]
    block = 16

    def fill(i, c):
        for u in range(8):
            t = i * 8 + u
            tok[row_ref[0, t]] = t
            tok[row_ref[1, t]] = t
        return c
    lax.fori_loop(0, tokens // 8, fill, 0)

    def relayout(i, c):
        r = pl.ds(pl.multiple_of(i * block, block), block)
        rows3[r] = x_ref[r].astype(F32).reshape(block, SUB, LANE).astype(BF16)
        return c
    lax.fori_loop(0, tokens // block, relayout, 0)

    slots = stage.shape[0]

    def copy(lane, slot):
        return pltpu.make_async_copy(stage.at[slot], out_ref.at[lane], sem.at[slot])

    def lane_step(lane, c):
        slot = lane % slots

        @pl.when(lane >= slots)
        def _():
            copy(lane - slots, slot).wait()

        def rows(i, c2):
            for u in range(8):
                r = i * 8 + u
                t = jnp.clip(tok[lane * size + r], 0, tokens - 1)
                stage[slot, r] = rows3[t]
            return c2
        lax.fori_loop(0, size // 8, rows, 0)
        copy(lane, slot).start()
        return c
    lax.fori_loop(0, lanes, lane_step, 0)
    for k in range(min(slots, lanes)):
        lane = lanes - min(slots, lanes) + k
        copy(lane, lane % slots).wait()


def ffn_kernel(size, cap_slot, start_ref, cnt_ref, core_ref, recv_ref, w1o, w1p, w2o, w2p, out_ref,
               recv_v, ret_v, w1_v, w2_v, xe, ze, x2, recv_sem, w_sem, out_sem):
    srcs = recv_ref.shape[0]
    exp_dev = w1o.shape[0]
    exp_chip = CORES * exp_dev
    core = core_ref[0]
    block = x2.shape[0]

    def recv_copy(s):
        return pltpu.make_async_copy(recv_ref.at[s], recv_v.at[pl.ds(s * size, size)], recv_sem.at[s])

    def out_copy(s):
        return pltpu.make_async_copy(ret_v.at[s, pl.ds(0, size)], out_ref.at[s], out_sem.at[s])

    def w_start(i):
        slot = i % 2
        local = i % exp_dev

        @pl.when(i // exp_dev == core)
        def _():
            pltpu.make_async_copy(w1o.at[local], w1_v.at[slot], w_sem.at[0, slot]).start()
            pltpu.make_async_copy(w2o.at[local], w2_v.at[slot], w_sem.at[1, slot]).start()

        @pl.when(i // exp_dev != core)
        def _():
            pltpu.make_async_copy(w1p.at[local], w1_v.at[slot], w_sem.at[0, slot]).start()
            pltpu.make_async_copy(w2p.at[local], w2_v.at[slot], w_sem.at[1, slot]).start()

    def w_wait(i):
        slot = i % 2
        pltpu.make_async_copy(w1o.at[0], w1_v.at[slot], w_sem.at[0, slot]).wait()
        pltpu.make_async_copy(w2o.at[0], w2_v.at[slot], w_sem.at[1, slot]).wait()

    for s in range(srcs):
        recv_copy(s).start()
    w_start(jnp.int32(0))
    for s in range(srcs):
        recv_copy(s).wait()

    def expert(i, c):
        slot = i % 2

        @pl.when(i + 1 < exp_chip)
        def _():
            w_start(i + 1)

        def gather(s, pos):
            n = cnt_ref[s, i]

            @pl.when(n > 0)
            def _():
                a = s * size + start_ref[s, i]
                for j in range(cap_slot):
                    xe[pos + j] = recv_v[a + j]
            return pos + n
        total = lax.fori_loop(0, srcs, gather, jnp.int32(0))
        w_wait(i)

        def tile(b, c2):
            base = pl.multiple_of(b * block, block)
            for q in range(block // 16):
                v = xe[pl.ds(base + q * 16, 16)].astype(F32).reshape(16, SUB * LANE)
                x2[pl.ds(q * 16, 16), :] = v.astype(BF16)
            h = jnp.dot(x2[...], w1_v[slot], preferred_element_type=F32)
            h = jax.nn.gelu(h, approximate=True).astype(BF16)
            z = jnp.dot(h, w2_v[slot], preferred_element_type=F32).astype(BF16).astype(F32)
            ze[pl.ds(base, block)] = z.reshape(block, SUB, LANE).astype(BF16)
            return c2
        lax.fori_loop(0, (total + block - 1) // block, tile, 0)

        def scatter(s, pos):
            n = cnt_ref[s, i]

            @pl.when(n > 0)
            def _():
                a = start_ref[s, i]
                for j in range(cap_slot):
                    ret_v[s, a + j] = ze[pos + j]
            return pos + n
        lax.fori_loop(0, srcs, scatter, jnp.int32(0))
        return c
    lax.fori_loop(0, exp_chip, expert, 0)
    for s in range(srcs):
        out_copy(s).start()
    for s in range(srcs):
        out_copy(s).wait()


def combine_kernel(row_ref, gate_ref, x_ref, ret_ref, out_ref, ret_v, y3, sem):
    tokens, d_model = x_ref.shape
    lanes, size = ret_ref.shape[:2]
    last = lanes * size - 1
    block = 16

    def copy(s):
        return pltpu.make_async_copy(ret_ref.at[s], ret_v.at[pl.ds(s * size, size)], sem.at[s])
    for s in range(lanes):
        copy(s).start()
    for s in range(lanes):
        copy(s).wait()

    def step(i, c):
        base = pl.multiple_of(i * block, block)
        for u in range(block):
            t = base + u
            g1 = gate_ref[0, t]
            g2 = gate_ref[1, t]
            z1 = ret_v[jnp.minimum(row_ref[0, t], last)].astype(F32)
            z2 = ret_v[jnp.minimum(row_ref[1, t], last)].astype(F32)
            y3[u] = jnp.where(g1 > 0, g1 * z1, 0.0) + jnp.where(g2 > 0, g2 * z2, 0.0)
        r = pl.ds(base, block)
        y = y3[...].reshape(block, d_model)
        out_ref[r, :] = (x_ref[r, :].astype(F32) + y).astype(BF16)
        return c
    lax.fori_loop(0, tokens // block, step, 0)


def spec(space):
    return pl.BlockSpec(memory_space=space)


SMEM = pltpu.SMEM
VMEM = pltpu.VMEM
ANY = pl.ANY


def params():
    return pltpu.CompilerParams(vmem_limit_bytes=VMEM_LIMIT)


def solution(mesh):
    devs = mesh.shape['ep']
    row_spec = P(('dp', 'ep'), None)
    expert_spec = P('ep', None, None)
    groups = [[i for i in range(devs) if i % CORES == c] for c in range(CORES)]
    partner = [(i, i ^ 1) for i in range(devs)]

    def local_step(x_rows, logits, w_in, w_out):
        tokens, d_model = x_rows.shape
        experts = logits.shape[1]
        exp_dev, _, hidden = w_in.shape
        capacity = CAP_FACTOR * tokens * devs // experts
        cap_slot = SLOT_FACTOR * tokens // experts
        exp_chip = CORES * exp_dev
        chips = devs // CORES
        full = exp_chip * cap_slot
        sizes = tuple(full * k // 32 for k in (21, 23, 32))
        me = lax.axis_index('ep').astype(I32)

        tok, gate, count = pl.pallas_call(
            route_kernel, name='route',
            out_shape=(jax.ShapeDtypeStruct((8, tokens), I32), jax.ShapeDtypeStruct((8, tokens), F32),
                       jax.ShapeDtypeStruct((8, experts), F32)),
            compiler_params=params())(logits)
        counts = lax.all_gather(count[0], 'ep')
        row, keep, start, cnt, pick = pl.pallas_call(
            functools.partial(plan_kernel, sizes, capacity, exp_dev), name='plan',
            out_shape=(jax.ShapeDtypeStruct((8, tokens), I32), jax.ShapeDtypeStruct((8, tokens), F32),
                       jax.ShapeDtypeStruct((chips, LANE), I32), jax.ShapeDtypeStruct((chips, LANE), I32),
                       jax.ShapeDtypeStruct((8, LANE), I32)),
            in_specs=[spec(SMEM)] + [spec(VMEM)] * 3,
            compiler_params=params())(me.reshape(1), counts, tok, gate)
        core = (me % CORES).reshape(1)

        def branch(size, x_rows, w_in, w_out, row, keep, start, cnt, core):
            lane_shape = jax.ShapeDtypeStruct((chips, size, SUB, LANE), BF16)
            w_in_p = lax.ppermute(w_in, 'ep', partner)
            w_out_p = lax.ppermute(w_out, 'ep', partner)
            send = pl.pallas_call(
                functools.partial(send_kernel, size), name='send', out_shape=lane_shape,
                in_specs=[spec(SMEM), spec(VMEM)], out_specs=spec(ANY),
                scratch_shapes=[SMEM((chips * size + 8,), I32), VMEM((tokens, SUB, LANE), BF16),
                                VMEM((4, size, SUB, LANE), BF16), pltpu.SemaphoreType.DMA((4,))],
                compiler_params=params())(row, x_rows)
            recv = lax.all_to_all(send, 'ep', 0, 0, axis_index_groups=groups, tiled=True)
            rows_max = capacity + cap_slot
            ret = pl.pallas_call(
                functools.partial(ffn_kernel, size, cap_slot), name='ffn', out_shape=lane_shape,
                in_specs=[spec(SMEM)] * 3 + [spec(ANY)] * 5, out_specs=spec(ANY),
                scratch_shapes=[
                    VMEM((chips * size + cap_slot, SUB, LANE), BF16),
                    VMEM((chips, size + cap_slot, SUB, LANE), BF16),
                    VMEM((2, d_model, hidden), BF16), VMEM((2, hidden, d_model), BF16),
                    VMEM((rows_max, SUB, LANE), BF16), VMEM((rows_max, SUB, LANE), BF16),
                    VMEM((LANE, d_model), BF16),
                    pltpu.SemaphoreType.DMA((chips,)), pltpu.SemaphoreType.DMA((2, 2)),
                    pltpu.SemaphoreType.DMA((chips,))],
                cost_estimate=pl.CostEstimate(flops=4 * chips * size * d_model * hidden,
                                              bytes_accessed=8 * exp_dev * d_model * hidden, transcendentals=0),
                compiler_params=params())(start, cnt, core, recv, w_in, w_in_p, w_out, w_out_p)
            back = lax.all_to_all(ret, 'ep', 0, 0, axis_index_groups=groups, tiled=True)
            return pl.pallas_call(
                combine_kernel, name='combine', out_shape=jax.ShapeDtypeStruct((tokens, d_model), BF16),
                in_specs=[spec(SMEM)] * 2 + [spec(VMEM), spec(ANY)], out_specs=spec(VMEM),
                scratch_shapes=[VMEM((chips * size, SUB, LANE), BF16), VMEM((16, SUB, LANE), F32),
                                pltpu.SemaphoreType.DMA((chips,))],
                compiler_params=params())(row, keep, x_rows, back)

        branches = [functools.partial(branch, size) for size in sizes]
        return lax.switch(pick[0, 0], branches, x_rows, w_in, w_out, row, keep, start, cnt, core)

    return jax.shard_map(local_step, mesh=mesh, in_specs=(row_spec, row_spec, expert_spec, expert_spec),
                         out_specs=row_spec, check_vma=False)
```

```python
import functools

import jax
import jax.numpy as jnp
from jax import lax
from jax.experimental import pallas as pl
from jax.experimental.pallas import tpu as pltpu
from jax.sharding import PartitionSpec as P

CAP_FACTOR = 2
SLOT_FACTOR = 4
CORES = 2
SUB = 16
LANE = 128
VMEM_LIMIT = 62 * 1024 * 1024
BF16 = jnp.bfloat16
F32 = jnp.float32
I32 = jnp.int32


MESH = pl.DeviceIdType.MESH


def iota(shape, dim):
    return lax.broadcasted_iota(I32, shape, dim)


def route_kernel(sizes, capacity, exp_dev, logits_ref, row_ref, keep_ref, start_ref, back_ref, pick_ref,
                 stage, counts_v, send_sem, recv_sem):
    tokens, experts = logits_ref.shape
    devs = counts_v.shape[0]
    exp_chip = CORES * exp_dev
    me = lax.axis_index('ep')
    chip = me // CORES
    core = me % CORES
    barrier = pltpu.get_barrier_semaphore()

    def other(d):
        return {'ep': (me + d) % devs}

    def hello(d, c):
        pl.semaphore_signal(barrier, inc=1, device_id=other(d), device_id_type=MESH)
        return c
    lax.fori_loop(1, devs, hello, 0)

    lt = logits_ref[...].T
    ids = iota(lt.shape, 0)
    m1 = jnp.max(lt, axis=0, keepdims=True)
    e1 = jnp.min(jnp.where(lt == m1, ids, experts), axis=0, keepdims=True)
    rest = jnp.where(ids == e1, -jnp.inf, lt)
    m2 = jnp.max(rest, axis=0, keepdims=True)
    e2 = jnp.min(jnp.where(rest == m2, ids, experts), axis=0, keepdims=True)
    hit1 = ids == e1
    hit2 = ids == e2
    chosen = jnp.where(hit1 | hit2, 1.0, 0.0).astype(BF16)
    ones = jnp.ones((8, tokens), BF16)
    count = lax.dot_general(ones, chosen, (((1,), (1,)), ((), ())), preferred_element_type=F32)
    stage[...] = count
    counts_v[me] = count
    pl.semaphore_wait(barrier, devs - 1)

    def copy(d):
        return pltpu.make_async_remote_copy(
            src_ref=stage, dst_ref=counts_v.at[me], send_sem=send_sem.at[d], recv_sem=recv_sem.at[d],
            device_id=other(d), device_id_type=MESH)

    def start_copy(d, c):
        copy(d).start()
        return c

    total = jnp.sum(jnp.exp(lt - m1), axis=0, keepdims=True)
    gates = (1.0 / total, jnp.exp(m2 - m1) / total)
    lax.fori_loop(1, devs, start_copy, 0)
    upper = jnp.where(iota((tokens, tokens), 0) < iota((tokens, tokens), 1), 1.0, 0.0).astype(BF16)
    before = jnp.dot(chosen, upper, preferred_element_type=F32)
    pos1 = jnp.sum(jnp.where(hit1, before, 0.0), axis=0, keepdims=True).astype(I32)
    pos2 = jnp.sum(jnp.where(hit2, before, 0.0), axis=0, keepdims=True).astype(I32)

    def wait_copy(d, c):
        copy(d).wait()
        return c
    lax.fori_loop(1, devs, wait_copy, 0)

    counts = counts_v[:, 0, :]
    lower = jnp.where(iota((devs, devs), 1) < iota((devs, devs), 0), 1.0, 0.0).astype(BF16)
    offs = jnp.dot(lower, counts.astype(BF16), preferred_element_type=F32)
    kept = jnp.minimum(jnp.maximum(capacity - offs, 0.0), counts)
    kept_b = kept.astype(BF16)
    row_e = iota((experts, experts), 0)
    col_e = iota((experts, experts), 1)
    same = (row_e // exp_chip == col_e // exp_chip) & (row_e < col_e)
    start = jnp.dot(kept_b, jnp.where(same, 1.0, 0.0).astype(BF16), preferred_element_type=F32)
    start_b = start.astype(BF16)
    member = jnp.where(iota((experts, LANE), 0) // exp_chip == iota((experts, LANE), 1), 1.0, 0.0).astype(BF16)
    totals = jnp.dot(kept_b, member, preferred_element_type=F32)
    most = jnp.max(jnp.max(totals, axis=0, keepdims=True), axis=1, keepdims=True).astype(I32)
    size = jnp.full((1, 1), sizes[0], I32)
    pick = jnp.zeros((1, 1), I32)
    for small, large in zip(sizes[:-1], sizes[1:]):
        size = jnp.where(most > small, large, size)
        pick = pick + jnp.where(most > small, 1, 0)
    pick_ref[...] = jnp.broadcast_to(pick, pick_ref.shape)

    mine = iota((devs, experts), 0) == me
    my_start = jnp.sum(jnp.where(mine, start, 0.0), axis=0, keepdims=True)
    my_kept = jnp.sum(jnp.where(mine, kept, 0.0), axis=0, keepdims=True)
    look = jnp.concatenate([my_start, my_kept, jnp.zeros((6, experts), F32)], axis=0).astype(BF16)
    lanes = experts // exp_chip
    for k, (e, hit, pos) in enumerate(((e1, hit1, pos1), (e2, hit2, pos2))):
        got = jnp.dot(look, jnp.where(hit, 1.0, 0.0).astype(BF16), preferred_element_type=F32).astype(I32)
        keep = pos < got[1:2, :]
        row = (e // exp_chip) * size + got[0:1, :] + pos
        row_ref[k:k + 1, :] = jnp.where(keep, row, lanes * size)
        keep_ref[k:k + 1, :] = jnp.where(keep, gates[k], 0.0)

    srcs = devs // CORES
    pick_src = jnp.where(iota((srcs, devs), 1) == CORES * iota((srcs, devs), 0) + core, 1.0, 0.0).astype(BF16)
    pick_exp = jnp.where(iota((exp_chip, experts), 1) == chip * exp_chip + iota((exp_chip, experts), 0),
                         1.0, 0.0).astype(BF16)
    contract = (((1,), (1,)), ((), ()))

    def mine_of(table):
        part = lax.dot_general(pick_exp, table, contract, preferred_element_type=F32).astype(BF16)
        return lax.dot_general(part, pick_src, contract, preferred_element_type=F32).astype(I32)
    first = mine_of(start_b)
    count = mine_of(kept_b)
    start_ref[...] = first
    width = back_ref.shape[1]
    ids = iota((exp_chip, width), 0)
    rows = iota((exp_chip, width), 1)
    group_rows = (srcs // 2) * capslot(tokens, experts)
    for s in range(srcs):
        off = rows - first[:, s:s + 1]
        inside = (off >= 0) & (off < count[:, s:s + 1])
        back_ref[s:s + 1, :] = jnp.sum(jnp.where(inside, ids * group_rows + off, 0), axis=0, keepdims=True)


def send_kernel(size, row_ref, x_ref, out_ref, tok, rows3, stage, sem):
    tokens, d_model = x_ref.shape
    lanes = out_ref.shape[0]
    block = 16

    def fill(i, c):
        for u in range(8):
            t = i * 8 + u
            tok[row_ref[0, t]] = t
            tok[row_ref[1, t]] = t
        return c
    lax.fori_loop(0, tokens // 8, fill, 0)

    def relayout(i, c):
        r = pl.ds(pl.multiple_of(i * block, block), block)
        rows3[r] = x_ref[r].astype(F32).reshape(block, SUB, LANE).astype(BF16)
        return c
    lax.fori_loop(0, tokens // block, relayout, 0)

    slots = stage.shape[0]

    def copy(lane, slot):
        return pltpu.make_async_copy(stage.at[slot], out_ref.at[lane], sem.at[slot])

    def lane_step(lane, c):
        slot = lane % slots

        @pl.when(lane >= slots)
        def _():
            copy(lane - slots, slot).wait()

        def rows(i, c2):
            for u in range(8):
                r = i * 8 + u
                t = jnp.clip(tok[lane * size + r], 0, tokens - 1)
                stage[slot, r] = rows3[t]
            return c2
        lax.fori_loop(0, size // 8, rows, 0)
        copy(lane, slot).start()
        return c
    lax.fori_loop(0, lanes, lane_step, 0)
    for k in range(min(slots, lanes)):
        lane = lanes - min(slots, lanes) + k
        copy(lane, lane % slots).wait()


def capslot(tokens, experts):
    return SLOT_FACTOR * tokens // experts


def grid_side(chips):
    return max(k for k in range(1, chips + 1) if chips % k == 0 and k * k <= chips)


def shifts_of(chips):
    side = grid_side(chips)
    steps = [(dy, dx) for dy in range(chips // side) for dx in range(side)]
    even = [s for s in steps if (s[0] + s[1]) % 2 == 0]
    odd = [s for s in steps if (s[0] + s[1]) % 2 == 1]
    order = even + odd
    half = chips // 2
    return order[:half], order[half:]


def moe_kernel(size, cap_slot, start_ref, map_ref, send_ref, w1o, w2o, back_ref, w1p, w2p,
               recv_a, recv_b, ret_v, ze, w1_v, w2_v, x2,
               out_sem, in_sem, ret_out_sem, ret_in_sem, swap_out_sem, swap_in_sem, w_sem):
    chips = send_ref.shape[0]
    exp_dev = w1o.shape[0]
    exp_chip = CORES * exp_dev
    groups = shifts_of(chips)
    half = len(groups[0])
    side = grid_side(chips)
    tall = chips // side
    me = lax.axis_index('ep')
    chip = me // CORES
    core = me % CORES
    cy = chip // side
    cx = chip % side
    partner = {'ep': chip * CORES + (1 - core)}

    def ahead(step):
        return ((cy + step[0]) % tall) * side + (cx + step[1]) % side

    def behind(step):
        return ((cy + tall - step[0]) % tall) * side + (cx + side - step[1]) % side

    def device(c):
        return {'ep': c * CORES + core}

    barrier = pltpu.get_barrier_semaphore()
    pl.semaphore_signal(barrier, inc=1, device_id=partner, device_id_type=MESH)
    for step in groups[0] + groups[1]:
        if step != (0, 0):
            pl.semaphore_signal(barrier, inc=1, device_id=device(ahead(step)), device_id_type=MESH)
    pl.semaphore_wait(barrier, chips)

    recvs = (recv_a, recv_b)

    def dispatch(g, q):
        step = groups[g][q]
        n = g * half + q
        dst = recvs[g].at[pl.ds(q * size, size)]
        if step == (0, 0):
            return pltpu.make_async_copy(send_ref.at[chip], dst, in_sem.at[n])
        to = ahead(step)
        return pltpu.make_async_remote_copy(
            src_ref=send_ref.at[to], dst_ref=dst, send_sem=out_sem.at[n], recv_sem=in_sem.at[n],
            device_id=device(to), device_id_type=MESH)

    def swap(k, j):
        src, dst = ((w1o, w1p), (w2o, w2p))[k]
        return pltpu.make_async_remote_copy(
            src_ref=src.at[j], dst_ref=dst.at[j], send_sem=swap_out_sem.at[k, j], recv_sem=swap_in_sem.at[k, j],
            device_id=partner, device_id_type=MESH)

    def give(g, q):
        step = groups[g][q]
        n = g * half + q
        src = ret_v.at[n]
        if step == (0, 0):
            return pltpu.make_async_copy(src, back_ref.at[chip], ret_in_sem.at[n])
        return pltpu.make_async_remote_copy(
            src_ref=src, dst_ref=back_ref.at[chip], send_sem=ret_out_sem.at[n], recv_sem=ret_in_sem.at[n],
            device_id=device(behind(step)), device_id_type=MESH)

    for g in range(2):
        for q in range(half):
            dispatch(g, q).start()

    def swap_start(j, c):
        swap(0, j).start()
        swap(1, j).start()
        return c
    lax.fori_loop(0, exp_dev, swap_start, 0)

    def load(a, b, j, slot):
        return (pltpu.make_async_copy(a.at[j], w1_v.at[slot], w_sem.at[0, slot]),
                pltpu.make_async_copy(b.at[j], w2_v.at[slot], w_sem.at[1, slot]))

    def load_start(a, b, j, slot):
        for d in load(a, b, j, slot):
            d.start()

    def load_wait(slot):
        for d in load(w1o, w2o, 0, slot):
            d.wait()

    def compute(g, i, slot):
        recv = recvs[g]
        for q in range(half):
            a = start_ref[i, behind(groups[g][q])] + q * size
            v = jnp.stack([recv[a + j] for j in range(cap_slot)]).astype(F32)
            x2[pl.ds(q * cap_slot, cap_slot), :] = v.reshape(cap_slot, SUB * LANE).astype(BF16)
        h = jnp.dot(x2[...], w1_v[slot], preferred_element_type=F32)
        h = jax.nn.gelu(h, approximate=True).astype(BF16)
        z = jnp.dot(h, w2_v[slot], preferred_element_type=F32).astype(BF16).astype(F32)
        rows = half * cap_slot
        ze[pl.ds(pl.multiple_of(i * rows, rows), rows)] = z.reshape(rows, SUB, LANE).astype(BF16)

    for g in range(2):
        load_start(w1o, w2o, 0, 0)
        for q in range(half):
            if groups[g][q] == (0, 0):
                dispatch(g, q).wait()
            else:
                dispatch(g, q).wait_recv()

        def own(j, c):
            slot = j % 2

            @pl.when(j + 1 < exp_dev)
            def _():
                load_start(w1o, w2o, j + 1, 1 - slot)
            load_wait(slot)
            compute(g, core * exp_dev + j, slot)
            return c
        lax.fori_loop(0, exp_dev, own, 0)

        def ready(j):
            if g == 0:
                swap(0, j).wait_recv()
                swap(1, j).wait_recv()
        ready(0)
        load_start(w1p, w2p, 0, 0)

        def theirs(j, c):
            slot = j % 2

            @pl.when(j + 1 < exp_dev)
            def _():
                ready(j + 1)
                load_start(w1p, w2p, j + 1, 1 - slot)
            load_wait(slot)
            compute(g, (1 - core) * exp_dev + j, slot)
            return c
        lax.fori_loop(0, exp_dev, theirs, 0)

        for q in range(half):
            lane = behind(groups[g][q])
            n = g * half + q

            def rows(b, c):
                for u in range(8):
                    r = b * 8 + u
                    ret_v[n, r] = ze[map_ref[lane, r] + q * cap_slot]
                return c
            lax.fori_loop(0, size // 8, rows, 0)
            if q > 0:
                give(g, q - 1).start()
        give(g, half - 1).start()

    def swap_end(j, c):
        swap(0, j).wait_send()
        swap(1, j).wait_send()
        return c
    lax.fori_loop(0, exp_dev, swap_end, 0)
    for g in range(2):
        for q in range(half):
            if groups[g][q] == (0, 0):
                give(g, q).wait()
            else:
                dispatch(g, q).wait_send()
                give(g, q).wait()


def combine_kernel(row_ref, gate_ref, x_ref, ret_ref, out_ref, ret_v, y3, sem):
    tokens, d_model = x_ref.shape
    lanes, size = ret_ref.shape[:2]
    last = lanes * size - 1
    block = 16

    def copy(s):
        return pltpu.make_async_copy(ret_ref.at[s], ret_v.at[pl.ds(s * size, size)], sem.at[s])
    for s in range(lanes):
        copy(s).start()
    for s in range(lanes):
        copy(s).wait()

    def step(i, c):
        base = pl.multiple_of(i * block, block)
        for u in range(block):
            t = base + u
            g1 = gate_ref[0, t]
            g2 = gate_ref[1, t]
            z1 = ret_v[jnp.minimum(row_ref[0, t], last)].astype(F32)
            z2 = ret_v[jnp.minimum(row_ref[1, t], last)].astype(F32)
            y3[u] = jnp.where(g1 > 0, g1 * z1, 0.0) + jnp.where(g2 > 0, g2 * z2, 0.0)
        r = pl.ds(base, block)
        y = y3[...].reshape(block, d_model)
        out_ref[r, :] = (x_ref[r, :].astype(F32) + y).astype(BF16)
        return c
    lax.fori_loop(0, tokens // block, step, 0)


def spec(space):
    return pl.BlockSpec(memory_space=space)


SMEM = pltpu.SMEM
VMEM = pltpu.VMEM
ANY = pl.ANY


def params(number=None):
    if number is None:
        return pltpu.CompilerParams(vmem_limit_bytes=VMEM_LIMIT)
    return pltpu.CompilerParams(vmem_limit_bytes=VMEM_LIMIT, collective_id=number, has_side_effects=True)


def solution(mesh):
    devs = mesh.shape['ep']
    row_spec = P(('dp', 'ep'), None)
    expert_spec = P('ep', None, None)

    def local_step(x_rows, logits, w_in, w_out):
        tokens, d_model = x_rows.shape
        experts = logits.shape[1]
        exp_dev, _, hidden = w_in.shape
        capacity = CAP_FACTOR * tokens * devs // experts
        cap_slot = capslot(tokens, experts)
        exp_chip = CORES * exp_dev
        chips = devs // CORES
        half = chips // 2
        full = exp_chip * cap_slot
        sizes = tuple(full * k // 32 for k in (21, 23, 32))

        row, keep, start, back_map, pick = pl.pallas_call(
            functools.partial(route_kernel, sizes, capacity, exp_dev), name='route',
            out_shape=(jax.ShapeDtypeStruct((8, tokens), I32), jax.ShapeDtypeStruct((8, tokens), F32),
                       jax.ShapeDtypeStruct((exp_chip, chips), I32), jax.ShapeDtypeStruct((chips, full), I32),
                       jax.ShapeDtypeStruct((8, LANE), I32)),
            in_specs=[spec(VMEM)],
            scratch_shapes=[VMEM((8, experts), F32), VMEM((devs, 8, experts), F32),
                            pltpu.SemaphoreType.DMA((devs,)), pltpu.SemaphoreType.DMA((devs,))],
            compiler_params=params(0))(logits)

        def branch(number, size, x_rows, w_in, w_out, row, keep, start, back_map):
            lane_shape = jax.ShapeDtypeStruct((chips, size, SUB, LANE), BF16)
            send = pl.pallas_call(
                functools.partial(send_kernel, size), name='send', out_shape=lane_shape,
                in_specs=[spec(SMEM), spec(VMEM)], out_specs=spec(ANY),
                scratch_shapes=[SMEM((chips * size + 8,), I32), VMEM((tokens, SUB, LANE), BF16),
                                VMEM((4, size, SUB, LANE), BF16), pltpu.SemaphoreType.DMA((4,))],
                compiler_params=params())(row, x_rows)
            dma = pltpu.SemaphoreType.DMA
            back, _, _ = pl.pallas_call(
                functools.partial(moe_kernel, size, cap_slot), name='moe',
                out_shape=(lane_shape, jax.ShapeDtypeStruct(w_in.shape, BF16),
                           jax.ShapeDtypeStruct(w_out.shape, BF16)),
                in_specs=[spec(SMEM)] * 2 + [spec(ANY)] * 3, out_specs=(spec(ANY),) * 3,
                scratch_shapes=[
                    VMEM((half * size + cap_slot, SUB, LANE), BF16),
                    VMEM((half * size + cap_slot, SUB, LANE), BF16),
                    VMEM((chips, size, SUB, LANE), BF16),
                    VMEM((exp_chip * half * cap_slot, SUB, LANE), BF16),
                    VMEM((2, d_model, hidden), BF16), VMEM((2, hidden, d_model), BF16),
                    VMEM((half * cap_slot, d_model), BF16),
                    dma((chips,)), dma((chips,)), dma((chips,)), dma((chips,)),
                    dma((2, exp_dev)), dma((2, exp_dev)), dma((2, 2))],
                compiler_params=params(number))(start, back_map, send, w_in, w_out)
            return pl.pallas_call(
                combine_kernel, name='combine', out_shape=jax.ShapeDtypeStruct((tokens, d_model), BF16),
                in_specs=[spec(SMEM)] * 2 + [spec(VMEM), spec(ANY)], out_specs=spec(VMEM),
                scratch_shapes=[VMEM((chips * size, SUB, LANE), BF16), VMEM((16, SUB, LANE), F32),
                                pltpu.SemaphoreType.DMA((chips,))],
                compiler_params=params())(row, keep, x_rows, back)

        branches = [functools.partial(branch, 1 + k, size) for k, size in enumerate(sizes)]
        return lax.switch(pick[0, 0], branches, x_rows, w_in, w_out, row, keep, start, back_map)

    return jax.shard_map(local_step, mesh=mesh, in_specs=(row_spec, row_spec, expert_spec, expert_spec),
                         out_specs=row_spec, check_vma=False)
```

```python
import functools

import jax
import jax.numpy as jnp
from jax import lax
from jax.experimental import pallas as pl
from jax.experimental.pallas import tpu as pltpu
from jax.sharding import PartitionSpec as P

CAP_FACTOR = 2
SLOT_FACTOR = 4
CORES = 2
SUB = 16
LANE = 128
VMEM_LIMIT = 62 * 1024 * 1024
BF16 = jnp.bfloat16
F32 = jnp.float32
I32 = jnp.int32


MESH = pl.DeviceIdType.MESH


def iota(shape, dim):
    return lax.broadcasted_iota(I32, shape, dim)


def route_kernel(sizes, capacity, exp_dev, logits_ref, row_ref, keep_ref, start_ref, cnt_ref, back_ref, pick_ref,
                 stage, counts_v, send_sem, recv_sem):
    tokens, experts = logits_ref.shape
    devs = counts_v.shape[0]
    exp_chip = CORES * exp_dev
    me = lax.axis_index('ep')
    chip = me // CORES
    core = me % CORES
    barrier = pltpu.get_barrier_semaphore()

    def other(d):
        return {'ep': (me + d) % devs}

    def hello(d, c):
        pl.semaphore_signal(barrier, inc=1, device_id=other(d), device_id_type=MESH)
        return c
    lax.fori_loop(1, devs, hello, 0)

    lt = logits_ref[...].T
    ids = iota(lt.shape, 0)
    m1 = jnp.max(lt, axis=0, keepdims=True)
    e1 = jnp.min(jnp.where(lt == m1, ids, experts), axis=0, keepdims=True)
    rest = jnp.where(ids == e1, -jnp.inf, lt)
    m2 = jnp.max(rest, axis=0, keepdims=True)
    e2 = jnp.min(jnp.where(rest == m2, ids, experts), axis=0, keepdims=True)
    hit1 = ids == e1
    hit2 = ids == e2
    chosen = jnp.where(hit1 | hit2, 1.0, 0.0).astype(BF16)
    ones = jnp.ones((8, tokens), BF16)
    count = lax.dot_general(ones, chosen, (((1,), (1,)), ((), ())), preferred_element_type=F32)
    stage[...] = count
    counts_v[me] = count
    pl.semaphore_wait(barrier, devs - 1)

    def copy(d):
        return pltpu.make_async_remote_copy(
            src_ref=stage, dst_ref=counts_v.at[me], send_sem=send_sem.at[d], recv_sem=recv_sem.at[d],
            device_id=other(d), device_id_type=MESH)

    def start_copy(d, c):
        copy(d).start()
        return c

    total = jnp.sum(jnp.exp(lt - m1), axis=0, keepdims=True)
    gates = (1.0 / total, jnp.exp(m2 - m1) / total)
    lax.fori_loop(1, devs, start_copy, 0)
    upper = jnp.where(iota((tokens, tokens), 0) < iota((tokens, tokens), 1), 1.0, 0.0).astype(BF16)
    before = jnp.dot(chosen, upper, preferred_element_type=F32)
    pos1 = jnp.sum(jnp.where(hit1, before, 0.0), axis=0, keepdims=True).astype(I32)
    pos2 = jnp.sum(jnp.where(hit2, before, 0.0), axis=0, keepdims=True).astype(I32)

    def wait_copy(d, c):
        copy(d).wait()
        return c
    lax.fori_loop(1, devs, wait_copy, 0)

    counts = counts_v[:, 0, :]
    lower = jnp.where(iota((devs, devs), 1) < iota((devs, devs), 0), 1.0, 0.0).astype(BF16)
    offs = jnp.dot(lower, counts.astype(BF16), preferred_element_type=F32)
    kept = jnp.minimum(jnp.maximum(capacity - offs, 0.0), counts)
    kept_b = kept.astype(BF16)
    row_e = iota((experts, experts), 0)
    col_e = iota((experts, experts), 1)
    same = (row_e // exp_chip == col_e // exp_chip) & (row_e < col_e)
    start = jnp.dot(kept_b, jnp.where(same, 1.0, 0.0).astype(BF16), preferred_element_type=F32)
    start_b = start.astype(BF16)
    member = jnp.where(iota((experts, LANE), 0) // exp_chip == iota((experts, LANE), 1), 1.0, 0.0).astype(BF16)
    totals = jnp.dot(kept_b, member, preferred_element_type=F32)
    most = jnp.max(jnp.max(totals, axis=0, keepdims=True), axis=1, keepdims=True).astype(I32)
    size = jnp.full((1, 1), sizes[0], I32)
    pick = jnp.zeros((1, 1), I32)
    for small, large in zip(sizes[:-1], sizes[1:]):
        size = jnp.where(most > small, large, size)
        pick = pick + jnp.where(most > small, 1, 0)
    pick_ref[...] = jnp.broadcast_to(pick, pick_ref.shape)

    mine = iota((devs, experts), 0) == me
    my_start = jnp.sum(jnp.where(mine, start, 0.0), axis=0, keepdims=True)
    my_kept = jnp.sum(jnp.where(mine, kept, 0.0), axis=0, keepdims=True)
    look = jnp.concatenate([my_start, my_kept, jnp.zeros((6, experts), F32)], axis=0).astype(BF16)
    lanes = experts // exp_chip
    for k, (e, hit, pos) in enumerate(((e1, hit1, pos1), (e2, hit2, pos2))):
        got = jnp.dot(look, jnp.where(hit, 1.0, 0.0).astype(BF16), preferred_element_type=F32).astype(I32)
        keep = pos < got[1:2, :]
        row = (e // exp_chip) * size + got[0:1, :] + pos
        row_ref[k:k + 1, :] = jnp.where(keep, row, lanes * size)
        keep_ref[k:k + 1, :] = jnp.where(keep, gates[k], 0.0)

    srcs = devs // CORES
    pick_src = jnp.where(iota((srcs, devs), 1) == CORES * iota((srcs, devs), 0) + core, 1.0, 0.0).astype(BF16)
    pick_exp = jnp.where(iota((exp_chip, experts), 1) == chip * exp_chip + iota((exp_chip, experts), 0),
                         1.0, 0.0).astype(BF16)
    contract = (((1,), (1,)), ((), ()))

    def mine_of(table):
        part = lax.dot_general(pick_exp, table, contract, preferred_element_type=F32).astype(BF16)
        return lax.dot_general(part, pick_src, contract, preferred_element_type=F32).astype(I32)
    first = mine_of(start_b)
    count = mine_of(kept_b)
    start_ref[...] = first
    cnt_ref[...] = count
    width = back_ref.shape[1]
    ids = iota((exp_chip, width), 0)
    rows = iota((exp_chip, width), 1)
    group_rows = (srcs // 2) * capslot(tokens, experts)
    for s in range(srcs):
        off = rows - first[:, s:s + 1]
        inside = (off >= 0) & (off < count[:, s:s + 1])
        back_ref[s:s + 1, :] = jnp.sum(jnp.where(inside, ids * group_rows + off, 0), axis=0, keepdims=True)


def unroll(size):
    return max(k for k in range(1, 33) if size % k == 0)


def send_kernel(size, row_ref, x_ref, out_ref, tok, x_v, rows3, stage, x_sem, sem):
    tokens, d_model = x_ref.shape
    lanes = out_ref.shape[0]
    block = 16
    parts = x_sem.shape[0]
    part = tokens // parts

    def x_copy(p):
        rows = pl.ds(p * part, part)
        return pltpu.make_async_copy(x_ref.at[rows], x_v.at[rows], x_sem.at[p])
    for p in range(parts):
        x_copy(p).start()

    def fill(i, c):
        for u in range(16):
            t = i * 16 + u
            tok[row_ref[0, t]] = t
            tok[row_ref[1, t]] = t
        return c
    lax.fori_loop(0, tokens // 16, fill, 0)

    def relayout(i, c):
        r = pl.ds(pl.multiple_of(i * block, block), block)
        rows3[r] = x_v[r].astype(F32).reshape(block, SUB, LANE).astype(BF16)
        return c
    for p in range(parts):
        x_copy(p).wait()
        lax.fori_loop(p * part // block, (p + 1) * part // block, relayout, 0)

    slots = stage.shape[0]
    step = unroll(size)

    def copy(lane, slot):
        return pltpu.make_async_copy(stage.at[slot], out_ref.at[lane], sem.at[slot])

    def lane_step(lane, c):
        slot = lane % slots

        @pl.when(lane >= slots)
        def _():
            copy(lane - slots, slot).wait()

        def rows(i, c2):
            for u in range(step):
                r = i * step + u
                t = tok[lane * size + r]
                t = t & (tokens - 1) if tokens & (tokens - 1) == 0 else jnp.clip(t, 0, tokens - 1)
                stage[slot, r] = rows3[t]
            return c2
        lax.fori_loop(0, size // step, rows, 0)
        copy(lane, slot).start()
        return c
    lax.fori_loop(0, lanes, lane_step, 0)
    for k in range(min(slots, lanes)):
        lane = lanes - min(slots, lanes) + k
        copy(lane, lane % slots).wait()


def capslot(tokens, experts):
    return SLOT_FACTOR * tokens // experts


def grid_side(chips):
    return max(k for k in range(1, chips + 1) if chips % k == 0 and k * k <= chips)


def shifts_of(chips):
    side = grid_side(chips)
    tall = chips // side
    steps = [(dy, dx) for dy in range(tall) for dx in range(side)]
    near = [s for s in steps if s != (0, 0) and 2 * s[0] != tall and 2 * s[1] != side]
    if 2 * len(near) != chips:
        near = [s for s in steps if (s[0] + s[1]) % 2 == 0]
    far = [s for s in steps if s not in near]
    far.sort(key=lambda s: relay_of(s, tall, side) is None)
    return near, far


def relay_of(step, tall, side):
    if 2 * step[1] == side and step[0] % 2 == 1:
        return (0, -1)
    if 2 * step[0] == tall and step[1] % 2 == 1:
        return (-1, 0)
    return None


def moe_kernel(size, cap_slot, start_ref, map_ref, send_ref, w1o, w2o, back_ref, w1p, w2p,
               recv_a, recv_b, ret_v, ze, w1_v, w2_v, x2, relay_v, relay_ret,
               relay_out, relay_in, relay_ret_out, relay_ret_in, out_sem, in_sem, ret_out_sem, ret_in_sem, swap_out_sem, swap_in_sem, w_sem):
    chips = send_ref.shape[0]
    exp_dev = w1o.shape[0]
    exp_chip = CORES * exp_dev
    groups = shifts_of(chips)
    half = len(groups[0])
    side = grid_side(chips)
    tall = chips // side
    me = lax.axis_index('ep')
    chip = me // CORES
    core = me % CORES
    cy = chip // side
    cx = chip % side
    partner = {'ep': chip * CORES + (1 - core)}

    def ahead(step):
        return ((cy + step[0]) % tall) * side + (cx + step[1]) % side

    def behind(step):
        return ((cy + tall - step[0]) % tall) * side + (cx + side - step[1]) % side

    def device(c):
        return {'ep': c * CORES + core}

    barrier = pltpu.get_barrier_semaphore()
    pl.semaphore_signal(barrier, inc=1, device_id=partner, device_id_type=MESH)
    for step in groups[0] + groups[1]:
        if step != (0, 0):
            pl.semaphore_signal(barrier, inc=1, device_id=device(ahead(step)), device_id_type=MESH)
    pl.semaphore_wait(barrier, chips)

    recvs = (recv_a, recv_b)

    relayed = [(g, q) for g in range(2) for q in range(half) if relay_of(groups[g][q], tall, side)]

    def via(g, q):
        return relay_of(groups[g][q], tall, side)

    def dispatch(g, q):
        step = groups[g][q]
        n = g * half + q
        dst = recvs[g].at[pl.ds(q * size, size)]
        if step == (0, 0):
            return pltpu.make_async_copy(send_ref.at[chip], dst, in_sem.at[n])
        if (g, q) in relayed:
            hop = via(g, q)
            src = relay_v.at[relayed.index((g, q))]
            to = ahead((step[0] - hop[0], step[1] - hop[1]))
        else:
            to = ahead(step)
            src = send_ref.at[to]
        return pltpu.make_async_remote_copy(
            src_ref=src, dst_ref=dst, send_sem=out_sem.at[n], recv_sem=in_sem.at[n],
            device_id=device(to), device_id_type=MESH)

    def dispatch_leg(g, q):
        r = relayed.index((g, q))
        return pltpu.make_async_remote_copy(
            src_ref=send_ref.at[ahead(groups[g][q])], dst_ref=relay_v.at[r], send_sem=relay_out.at[r],
            recv_sem=relay_in.at[r], device_id=device(ahead(via(g, q))), device_id_type=MESH)

    def swap(k, j):
        src, dst = ((w1o, w1p), (w2o, w2p))[k]
        return pltpu.make_async_remote_copy(
            src_ref=src.at[j], dst_ref=dst.at[j], send_sem=swap_out_sem.at[k, j], recv_sem=swap_in_sem.at[k, j],
            device_id=partner, device_id_type=MESH)

    def give(g, q):
        step = groups[g][q]
        n = g * half + q
        src = ret_v.at[n]
        home = chip
        to = behind(step)
        if step == (0, 0):
            return pltpu.make_async_copy(src, back_ref.at[chip], ret_in_sem.at[n])
        if (g, q) in relayed:
            hop = via(g, q)
            src = relay_ret.at[relayed.index((g, q))]
            home = behind(hop)
            to = behind((step[0] + hop[0], step[1] + hop[1]))
        return pltpu.make_async_remote_copy(
            src_ref=src, dst_ref=back_ref.at[home], send_sem=ret_out_sem.at[n], recv_sem=ret_in_sem.at[n],
            device_id=device(to), device_id_type=MESH)

    def give_leg(g, q):
        r = relayed.index((g, q))
        return pltpu.make_async_remote_copy(
            src_ref=ret_v.at[g * half + q], dst_ref=relay_ret.at[r], send_sem=relay_ret_out.at[r],
            recv_sem=relay_ret_in.at[r], device_id=device(ahead(via(g, q))), device_id_type=MESH)

    def give_start(g, q):
        if (g, q) in relayed:
            give_leg(g, q).start()
        else:
            give(g, q).start()

    for g, q in relayed:
        dispatch_leg(g, q).start()
    for g in range(2):
        for q in range(half):
            if (g, q) not in relayed:
                dispatch(g, q).start()

    def swap_start(j, c):
        swap(0, j).start()
        swap(1, j).start()
        return c
    lax.fori_loop(0, exp_dev, swap_start, 0)
    for g, q in relayed:
        dispatch_leg(g, q).wait_recv()
        dispatch(g, q).start()

    def load(a, b, j, slot):
        return (pltpu.make_async_copy(a.at[j], w1_v.at[slot], w_sem.at[0, slot]),
                pltpu.make_async_copy(b.at[j], w2_v.at[slot], w_sem.at[1, slot]))

    def load_start(a, b, j, slot):
        for d in load(a, b, j, slot):
            d.start()

    def load_wait(slot):
        for d in load(w1o, w2o, 0, slot):
            d.wait()

    def compute(g, i, slot):
        recv = recvs[g]
        for q in range(half):
            a = start_ref[i, behind(groups[g][q])] + q * size
            v = jnp.stack([recv[a + j] for j in range(cap_slot)]).astype(F32)
            x2[pl.ds(q * cap_slot, cap_slot), :] = v.reshape(cap_slot, SUB * LANE).astype(BF16)
        h = jnp.dot(x2[...], w1_v[slot], preferred_element_type=F32)
        h = jax.nn.gelu(h, approximate=True).astype(BF16)
        z = jnp.dot(h, w2_v[slot], preferred_element_type=F32).astype(BF16).astype(F32)
        rows = half * cap_slot
        ze[pl.ds(pl.multiple_of(i * rows, rows), rows)] = z.reshape(rows, SUB, LANE).astype(BF16)

    for g in range(2):
        load_start(w1o, w2o, 0, 0)
        for q in range(half):
            if groups[g][q] == (0, 0):
                dispatch(g, q).wait()
            else:
                dispatch(g, q).wait_recv()

        def own(j, c):
            slot = j % 2

            @pl.when(j + 1 < exp_dev)
            def _():
                load_start(w1o, w2o, j + 1, 1 - slot)
            load_wait(slot)
            compute(g, core * exp_dev + j, slot)
            return c
        lax.fori_loop(0, exp_dev, own, 0)

        def ready(j):
            if g == 0:
                swap(0, j).wait_recv()
                swap(1, j).wait_recv()
        ready(0)
        load_start(w1p, w2p, 0, 0)

        def theirs(j, c):
            slot = j % 2

            @pl.when(j + 1 < exp_dev)
            def _():
                ready(j + 1)
                load_start(w1p, w2p, j + 1, 1 - slot)
            load_wait(slot)
            compute(g, (1 - core) * exp_dev + j, slot)
            return c
        lax.fori_loop(0, exp_dev, theirs, 0)

        for q in range(half):
            lane = behind(groups[g][q])
            n = g * half + q

            def rows(b, c):
                for u in range(unroll(size)):
                    r = b * unroll(size) + u
                    ret_v[n, r] = ze[map_ref[lane, r] + q * cap_slot]
                return c
            lax.fori_loop(0, size // unroll(size), rows, 0)
            if q > 0:
                give_start(g, q - 1)
        give_start(g, half - 1)

    for g, q in relayed:
        give_leg(g, q).wait_recv()
        give(g, q).start()
        give_leg(g, q).wait_send()
        dispatch_leg(g, q).wait_send()

    def swap_end(j, c):
        swap(0, j).wait_send()
        swap(1, j).wait_send()
        return c
    lax.fori_loop(0, exp_dev, swap_end, 0)
    for g in range(2):
        for q in range(half):
            if groups[g][q] == (0, 0):
                give(g, q).wait()
            else:
                dispatch(g, q).wait_send()
                give(g, q).wait()


def ffn_kernel(size, cap_slot, start_ref, cnt_ref, core_ref, recv_ref, w1o, w1p, w2o, w2p, out_ref,
               recv_v, ret_v, w1_v, w2_v, xe, ze, x2, recv_sem, w_sem, out_sem):
    srcs = recv_ref.shape[0]
    exp_dev = w1o.shape[0]
    exp_chip = CORES * exp_dev
    core = core_ref[0]
    block = x2.shape[0]

    def recv_copy(s):
        return pltpu.make_async_copy(recv_ref.at[s], recv_v.at[pl.ds(s * size, size)], recv_sem.at[s])

    def out_copy(s):
        return pltpu.make_async_copy(ret_v.at[s, pl.ds(0, size)], out_ref.at[s], out_sem.at[s])

    def w_start(i):
        slot = i % 2
        local = i % exp_dev

        @pl.when(i // exp_dev == core)
        def _():
            pltpu.make_async_copy(w1o.at[local], w1_v.at[slot], w_sem.at[0, slot]).start()
            pltpu.make_async_copy(w2o.at[local], w2_v.at[slot], w_sem.at[1, slot]).start()

        @pl.when(i // exp_dev != core)
        def _():
            pltpu.make_async_copy(w1p.at[local], w1_v.at[slot], w_sem.at[0, slot]).start()
            pltpu.make_async_copy(w2p.at[local], w2_v.at[slot], w_sem.at[1, slot]).start()

    def w_wait(i):
        slot = i % 2
        pltpu.make_async_copy(w1o.at[0], w1_v.at[slot], w_sem.at[0, slot]).wait()
        pltpu.make_async_copy(w2o.at[0], w2_v.at[slot], w_sem.at[1, slot]).wait()

    for s in range(srcs):
        recv_copy(s).start()
    w_start(jnp.int32(0))
    for s in range(srcs):
        recv_copy(s).wait()

    def expert(i, c):
        slot = i % 2

        @pl.when(i + 1 < exp_chip)
        def _():
            w_start(i + 1)

        def gather(s, pos):
            n = cnt_ref[i, s]

            @pl.when(n > 0)
            def _():
                a = s * size + start_ref[i, s]
                for j in range(cap_slot):
                    xe[pos + j] = recv_v[a + j]
            return pos + n
        total = lax.fori_loop(0, srcs, gather, jnp.int32(0))
        w_wait(i)

        def tile(b, c2):
            base = pl.multiple_of(b * block, block)
            for q in range(block // 16):
                v = xe[pl.ds(base + q * 16, 16)].astype(F32).reshape(16, SUB * LANE)
                x2[pl.ds(q * 16, 16), :] = v.astype(BF16)
            h = jnp.dot(x2[...], w1_v[slot], preferred_element_type=F32)
            h = jax.nn.gelu(h, approximate=True).astype(BF16)
            z = jnp.dot(h, w2_v[slot], preferred_element_type=F32).astype(BF16).astype(F32)
            ze[pl.ds(base, block)] = z.reshape(block, SUB, LANE).astype(BF16)
            return c2
        lax.fori_loop(0, (total + block - 1) // block, tile, 0)

        def scatter(s, pos):
            n = cnt_ref[i, s]

            @pl.when(n > 0)
            def _():
                a = start_ref[i, s]
                for j in range(cap_slot):
                    ret_v[s, a + j] = ze[pos + j]
            return pos + n
        lax.fori_loop(0, srcs, scatter, jnp.int32(0))
        return c
    lax.fori_loop(0, exp_chip, expert, 0)
    for s in range(srcs):
        out_copy(s).start()
    for s in range(srcs):
        out_copy(s).wait()


def combine_kernel(row_ref, gate_ref, x_ref, ret_ref, out_ref, ret_v, x_v, out_v, y3, sem, x_sem, out_sem):
    tokens, d_model = x_ref.shape
    lanes, size = ret_ref.shape[:2]
    last = lanes * size - 1
    block = 16
    parts = x_sem.shape[0]
    part = tokens // parts

    def copy(s):
        return pltpu.make_async_copy(ret_ref.at[s], ret_v.at[pl.ds(s * size, size)], sem.at[s])

    def x_copy(p):
        rows = pl.ds(p * part, part)
        return pltpu.make_async_copy(x_ref.at[rows], x_v.at[rows], x_sem.at[p])

    def out_copy(p):
        rows = pl.ds(p * part, part)
        return pltpu.make_async_copy(out_v.at[rows], out_ref.at[rows], out_sem.at[p])
    for s in range(lanes):
        copy(s).start()
    for p in range(parts):
        x_copy(p).start()
    for s in range(lanes):
        copy(s).wait()

    def step(i, c):
        base = pl.multiple_of(i * block, block)
        for u in range(block):
            t = base + u
            g1 = gate_ref[0, t]
            g2 = gate_ref[1, t]
            z1 = ret_v[jnp.minimum(row_ref[0, t], last)].astype(F32)
            z2 = ret_v[jnp.minimum(row_ref[1, t], last)].astype(F32)
            y3[u] = jnp.where(g1 > 0, g1 * z1, 0.0) + jnp.where(g2 > 0, g2 * z2, 0.0)
        r = pl.ds(base, block)
        y = y3[...].reshape(block, d_model)
        out_v[r, :] = (x_v[r, :].astype(F32) + y).astype(BF16)
        return c
    for p in range(parts):
        x_copy(p).wait()
        lax.fori_loop(p * part // block, (p + 1) * part // block, step, 0)
        out_copy(p).start()
    for p in range(parts):
        out_copy(p).wait()


def spec(space):
    return pl.BlockSpec(memory_space=space)


SMEM = pltpu.SMEM
VMEM = pltpu.VMEM
ANY = pl.ANY


def params(number=None):
    if number is None:
        return pltpu.CompilerParams(vmem_limit_bytes=VMEM_LIMIT)
    return pltpu.CompilerParams(vmem_limit_bytes=VMEM_LIMIT, collective_id=number, has_side_effects=True)


def solution(mesh):
    devs = mesh.shape['ep']
    row_spec = P(('dp', 'ep'), None)
    expert_spec = P('ep', None, None)
    classes = [[i for i in range(devs) if i % CORES == c] for c in range(CORES)]
    partner = [(i, i ^ 1) for i in range(devs)]
    dma = pltpu.SemaphoreType.DMA

    def local_step(x_rows, logits, w_in, w_out):
        tokens, d_model = x_rows.shape
        experts = logits.shape[1]
        exp_dev, _, hidden = w_in.shape
        capacity = CAP_FACTOR * tokens * devs // experts
        cap_slot = capslot(tokens, experts)
        exp_chip = CORES * exp_dev
        chips = devs // CORES
        half = chips // 2
        full = exp_chip * cap_slot
        sizes = tuple(full * k // 32 for k in (21, 22, 32))
        core = (lax.axis_index('ep').astype(I32) % CORES).reshape(1)

        row, keep, start, cnt, back_map, pick = pl.pallas_call(
            functools.partial(route_kernel, sizes, capacity, exp_dev), name='route',
            out_shape=(jax.ShapeDtypeStruct((8, tokens), I32), jax.ShapeDtypeStruct((8, tokens), F32),
                       jax.ShapeDtypeStruct((exp_chip, chips), I32), jax.ShapeDtypeStruct((exp_chip, chips), I32),
                       jax.ShapeDtypeStruct((chips, full), I32), jax.ShapeDtypeStruct((8, LANE), I32)),
            in_specs=[spec(VMEM)],
            scratch_shapes=[VMEM((8, experts), F32), VMEM((devs, 8, experts), F32), dma((devs,)), dma((devs,))],
            compiler_params=params(0))(logits)

        def pack(size, row, x_rows):
            return pl.pallas_call(
                functools.partial(send_kernel, size), name='send',
                out_shape=jax.ShapeDtypeStruct((chips, size, SUB, LANE), BF16),
                in_specs=[spec(SMEM), spec(ANY)], out_specs=spec(ANY),
                scratch_shapes=[SMEM((chips * size + 8,), I32), VMEM((tokens, d_model), BF16),
                                VMEM((tokens, SUB, LANE), BF16), VMEM((4, size, SUB, LANE), BF16),
                                dma((4,)), dma((4,))],
                compiler_params=params())(row, x_rows)

        def combine(size, row, keep, x_rows, back):
            return pl.pallas_call(
                combine_kernel, name='combine', out_shape=jax.ShapeDtypeStruct((tokens, d_model), BF16),
                in_specs=[spec(SMEM)] * 2 + [spec(ANY)] * 2, out_specs=spec(ANY),
                scratch_shapes=[VMEM((chips * size, SUB, LANE), BF16), VMEM((tokens, d_model), BF16),
                                VMEM((tokens, d_model), BF16), VMEM((16, SUB, LANE), F32),
                                dma((chips,)), dma((4,)), dma((4,))],
                compiler_params=params())(row, keep, x_rows, back)

        def fused(number, size, x_rows, w_in, w_out, row, keep, start, cnt, back_map):
            lane_shape = jax.ShapeDtypeStruct((chips, size, SUB, LANE), BF16)
            send = pack(size, row, x_rows)
            near, far = shifts_of(chips)
            side = grid_side(chips)
            relays = max(1, sum(relay_of(s, chips // side, side) is not None for s in near + far))
            back, _, _ = pl.pallas_call(
                functools.partial(moe_kernel, size, cap_slot), name='moe',
                out_shape=(lane_shape, jax.ShapeDtypeStruct(w_in.shape, BF16),
                           jax.ShapeDtypeStruct(w_out.shape, BF16)),
                in_specs=[spec(SMEM)] * 2 + [spec(ANY)] * 3, out_specs=(spec(ANY),) * 3,
                scratch_shapes=[
                    VMEM((half * size + cap_slot, SUB, LANE), BF16),
                    VMEM((half * size + cap_slot, SUB, LANE), BF16),
                    VMEM((chips, size, SUB, LANE), BF16),
                    VMEM((exp_chip * half * cap_slot, SUB, LANE), BF16),
                    VMEM((2, d_model, hidden), BF16), VMEM((2, hidden, d_model), BF16),
                    VMEM((half * cap_slot, d_model), BF16),
                    VMEM((relays, size, SUB, LANE), BF16), VMEM((relays, size, SUB, LANE), BF16),
                    dma((relays,)), dma((relays,)), dma((relays,)), dma((relays,)),
                    dma((chips,)), dma((chips,)), dma((chips,)), dma((chips,)),
                    dma((2, exp_dev)), dma((2, exp_dev)), dma((2, 2))],
                compiler_params=params(number))(start, back_map, send, w_in, w_out)
            return combine(size, row, keep, x_rows, back)

        def general(size, x_rows, w_in, w_out, row, keep, start, cnt, back_map):
            w_in_p = lax.ppermute(w_in, 'ep', partner)
            w_out_p = lax.ppermute(w_out, 'ep', partner)
            send = pack(size, row, x_rows)
            recv = lax.all_to_all(send, 'ep', 0, 0, axis_index_groups=classes, tiled=True)
            rows_max = capacity + cap_slot
            ret = pl.pallas_call(
                functools.partial(ffn_kernel, size, cap_slot), name='ffn',
                out_shape=jax.ShapeDtypeStruct((chips, size, SUB, LANE), BF16),
                in_specs=[spec(SMEM)] * 3 + [spec(ANY)] * 5, out_specs=spec(ANY),
                scratch_shapes=[
                    VMEM((chips * size + cap_slot, SUB, LANE), BF16),
                    VMEM((chips, size + cap_slot, SUB, LANE), BF16),
                    VMEM((2, d_model, hidden), BF16), VMEM((2, hidden, d_model), BF16),
                    VMEM((rows_max, SUB, LANE), BF16), VMEM((rows_max, SUB, LANE), BF16),
                    VMEM((LANE, d_model), BF16), dma((chips,)), dma((2, 2)), dma((chips,))],
                compiler_params=params())(start, cnt, core, recv, w_in, w_in_p, w_out, w_out_p)
            back = lax.all_to_all(ret, 'ep', 0, 0, axis_index_groups=classes, tiled=True)
            return combine(size, row, keep, x_rows, back)

        branches = [functools.partial(fused, 1 + k, size) for k, size in enumerate(sizes[:-1])]
        branches.append(functools.partial(general, sizes[-1]))
        return lax.switch(pick[0, 0], branches, x_rows, w_in, w_out, row, keep, start, cnt, back_map)

    return jax.shard_map(local_step, mesh=mesh, in_specs=(row_spec, row_spec, expert_spec, expert_spec),
                         out_specs=row_spec, check_vma=False)
```

```python
import functools

import jax
import jax.numpy as jnp
from jax import lax
from jax.experimental import pallas as pl
from jax.experimental.pallas import tpu as pltpu
from jax.sharding import PartitionSpec as P

CAP_FACTOR = 2
SLOT_FACTOR = 4
CORES = 2
SUB = 16
LANE = 128
VMEM_LIMIT = 62 * 1024 * 1024
BF16 = jnp.bfloat16
F32 = jnp.float32
I32 = jnp.int32


MESH = pl.DeviceIdType.MESH


def iota(shape, dim):
    return lax.broadcasted_iota(I32, shape, dim)


def route_kernel(sizes, capacity, exp_dev, logits_ref, row_ref, keep_ref, start_ref, cnt_ref, back_ref, pick_ref,
                 stage, counts_v, send_sem, recv_sem):
    tokens, experts = logits_ref.shape
    devs = counts_v.shape[0]
    exp_chip = CORES * exp_dev
    me = lax.axis_index('ep')
    chip = me // CORES
    core = me % CORES
    barrier = pltpu.get_barrier_semaphore()

    def other(d):
        return {'ep': (me + d) % devs}

    def hello(d, c):
        pl.semaphore_signal(barrier, inc=1, device_id=other(d), device_id_type=MESH)
        return c
    lax.fori_loop(1, devs, hello, 0)

    lt = logits_ref[...].T
    ids = iota(lt.shape, 0)
    m1 = jnp.max(lt, axis=0, keepdims=True)
    e1 = jnp.min(jnp.where(lt == m1, ids, experts), axis=0, keepdims=True)
    rest = jnp.where(ids == e1, -jnp.inf, lt)
    m2 = jnp.max(rest, axis=0, keepdims=True)
    e2 = jnp.min(jnp.where(rest == m2, ids, experts), axis=0, keepdims=True)
    hit1 = ids == e1
    hit2 = ids == e2
    chosen = jnp.where(hit1 | hit2, 1.0, 0.0).astype(BF16)
    ones = jnp.ones((8, tokens), BF16)
    count = lax.dot_general(ones, chosen, (((1,), (1,)), ((), ())), preferred_element_type=F32)
    stage[...] = count
    counts_v[me] = count
    pl.semaphore_wait(barrier, devs - 1)

    def copy(d):
        return pltpu.make_async_remote_copy(
            src_ref=stage, dst_ref=counts_v.at[me], send_sem=send_sem.at[d], recv_sem=recv_sem.at[d],
            device_id=other(d), device_id_type=MESH)

    def start_copy(d, c):
        copy(d).start()
        return c

    total = jnp.sum(jnp.exp(lt - m1), axis=0, keepdims=True)
    gates = (1.0 / total, jnp.exp(m2 - m1) / total)
    lax.fori_loop(1, devs, start_copy, 0)
    upper = jnp.where(iota((tokens, tokens), 0) < iota((tokens, tokens), 1), 1.0, 0.0).astype(BF16)
    before = jnp.dot(chosen, upper, preferred_element_type=F32)
    pos1 = jnp.sum(jnp.where(hit1, before, 0.0), axis=0, keepdims=True).astype(I32)
    pos2 = jnp.sum(jnp.where(hit2, before, 0.0), axis=0, keepdims=True).astype(I32)

    def wait_copy(d, c):
        copy(d).wait()
        return c
    lax.fori_loop(1, devs, wait_copy, 0)

    counts = counts_v[:, 0, :]
    lower = jnp.where(iota((devs, devs), 1) < iota((devs, devs), 0), 1.0, 0.0).astype(BF16)
    offs = jnp.dot(lower, counts.astype(BF16), preferred_element_type=F32)
    kept = jnp.minimum(jnp.maximum(capacity - offs, 0.0), counts)
    kept_b = kept.astype(BF16)
    row_e = iota((experts, experts), 0)
    col_e = iota((experts, experts), 1)
    same = (row_e // exp_chip == col_e // exp_chip) & (row_e < col_e)
    start = jnp.dot(kept_b, jnp.where(same, 1.0, 0.0).astype(BF16), preferred_element_type=F32)
    start_b = start.astype(BF16)
    member = jnp.where(iota((experts, LANE), 0) // exp_chip == iota((experts, LANE), 1), 1.0, 0.0).astype(BF16)
    totals = jnp.dot(kept_b, member, preferred_element_type=F32)
    most = jnp.max(jnp.max(totals, axis=0, keepdims=True), axis=1, keepdims=True).astype(I32)
    size = jnp.full((1, 1), sizes[0], I32)
    pick = jnp.zeros((1, 1), I32)
    for small, large in zip(sizes[:-1], sizes[1:]):
        size = jnp.where(most > small, large, size)
        pick = pick + jnp.where(most > small, 1, 0)
    pick_ref[...] = jnp.broadcast_to(pick, pick_ref.shape)

    mine = iota((devs, experts), 0) == me
    my_start = jnp.sum(jnp.where(mine, start, 0.0), axis=0, keepdims=True)
    my_kept = jnp.sum(jnp.where(mine, kept, 0.0), axis=0, keepdims=True)
    look = jnp.concatenate([my_start, my_kept, jnp.zeros((6, experts), F32)], axis=0).astype(BF16)
    lanes = experts // exp_chip
    for k, (e, hit, pos) in enumerate(((e1, hit1, pos1), (e2, hit2, pos2))):
        got = jnp.dot(look, jnp.where(hit, 1.0, 0.0).astype(BF16), preferred_element_type=F32).astype(I32)
        keep = pos < got[1:2, :]
        row = (e // exp_chip) * size + got[0:1, :] + pos
        row_ref[k:k + 1, :] = jnp.where(keep, row, lanes * size)
        keep_ref[k:k + 1, :] = jnp.where(keep, gates[k], 0.0)

    srcs = devs // CORES
    pick_src = jnp.where(iota((srcs, devs), 1) == CORES * iota((srcs, devs), 0) + core, 1.0, 0.0).astype(BF16)
    pick_exp = jnp.where(iota((exp_chip, experts), 1) == chip * exp_chip + iota((exp_chip, experts), 0),
                         1.0, 0.0).astype(BF16)
    contract = (((1,), (1,)), ((), ()))

    def mine_of(table):
        part = lax.dot_general(pick_exp, table, contract, preferred_element_type=F32).astype(BF16)
        return lax.dot_general(part, pick_src, contract, preferred_element_type=F32).astype(I32)
    first = mine_of(start_b)
    count = mine_of(kept_b)
    start_ref[...] = first
    cnt_ref[...] = count
    width = back_ref.shape[1]
    ids = iota((exp_chip, width), 0)
    rows = iota((exp_chip, width), 1)
    group_rows = (srcs // 2) * capslot(tokens, experts)
    for s in range(srcs):
        off = rows - first[:, s:s + 1]
        inside = (off >= 0) & (off < count[:, s:s + 1])
        back_ref[s:s + 1, :] = jnp.sum(jnp.where(inside, ids * group_rows + off, 0), axis=0, keepdims=True)


def unroll(size):
    return max(k for k in range(1, 33) if size % k == 0)


def send_kernel(size, row_ref, x_ref, out_ref, tok, x_v, rows3, stage, x_sem, sem):
    tokens, d_model = x_ref.shape
    lanes = out_ref.shape[0]
    block = 16
    parts = x_sem.shape[0]
    part = tokens // parts

    def x_copy(p):
        rows = pl.ds(p * part, part)
        return pltpu.make_async_copy(x_ref.at[rows], x_v.at[rows], x_sem.at[p])
    for p in range(parts):
        x_copy(p).start()

    def fill(i, c):
        for u in range(16):
            t = i * 16 + u
            tok[row_ref[0, t]] = t
            tok[row_ref[1, t]] = t
        return c
    lax.fori_loop(0, tokens // 16, fill, 0)

    def relayout(i, c):
        r = pl.ds(pl.multiple_of(i * block, block), block)
        rows3[r] = x_v[r].astype(F32).reshape(block, SUB, LANE).astype(BF16)
        return c
    for p in range(parts):
        x_copy(p).wait()
        lax.fori_loop(p * part // block, (p + 1) * part // block, relayout, 0)

    slots = stage.shape[0]
    step = unroll(size)

    def copy(lane, slot):
        return pltpu.make_async_copy(stage.at[slot], out_ref.at[lane], sem.at[slot])

    def lane_step(lane, c):
        slot = lane % slots

        @pl.when(lane >= slots)
        def _():
            copy(lane - slots, slot).wait()

        def rows(i, c2):
            for u in range(step):
                r = i * step + u
                t = tok[lane * size + r]
                t = t & (tokens - 1) if tokens & (tokens - 1) == 0 else jnp.clip(t, 0, tokens - 1)
                stage[slot, r] = rows3[t]
            return c2
        lax.fori_loop(0, size // step, rows, 0)
        copy(lane, slot).start()
        return c
    lax.fori_loop(0, lanes, lane_step, 0)
    for k in range(min(slots, lanes)):
        lane = lanes - min(slots, lanes) + k
        copy(lane, lane % slots).wait()


def capslot(tokens, experts):
    return SLOT_FACTOR * tokens // experts


def grid_side(chips):
    return max(k for k in range(1, chips + 1) if chips % k == 0 and k * k <= chips)


def shifts_of(chips):
    side = grid_side(chips)
    tall = chips // side
    steps = [(dy, dx) for dy in range(tall) for dx in range(side)]
    near = [s for s in steps if s != (0, 0) and 2 * s[0] != tall and 2 * s[1] != side]
    if 2 * len(near) != chips:
        near = [s for s in steps if (s[0] + s[1]) % 2 == 0]
    far = [s for s in steps if s not in near]
    turn = (tall - 1) * (side - 1) + 1

    def rank(s):
        return (0 in s, s == (0, 0), s[1] == 0, (s[0] * turn + s[1]) % 2, s[0] != s[1])
    return sorted(near, key=rank), sorted(far, key=rank)


def moe_kernel(size, cap_slot, start_ref, map_ref, send_ref, w1o, w2o, back_ref, w1p, w2p,
               recv_a, recv_b, ret_v, ze, w1_v, w2_v, x2,
               out_sem, in_sem, ret_out_sem, ret_in_sem, swap_out_sem, swap_in_sem, w_sem):
    chips = send_ref.shape[0]
    exp_dev = w1o.shape[0]
    exp_chip = CORES * exp_dev
    groups = shifts_of(chips)
    half = len(groups[0])
    side = grid_side(chips)
    tall = chips // side
    me = lax.axis_index('ep')
    chip = me // CORES
    core = me % CORES
    cy = chip // side
    cx = chip % side
    partner = {'ep': chip * CORES + (1 - core)}

    def ahead(step):
        return ((cy + step[0]) % tall) * side + (cx + step[1]) % side

    def behind(step):
        return ((cy + tall - step[0]) % tall) * side + (cx + side - step[1]) % side

    def device(c):
        return {'ep': c * CORES + core}

    barrier = pltpu.get_barrier_semaphore()
    pl.semaphore_signal(barrier, inc=1, device_id=partner, device_id_type=MESH)
    for step in groups[0] + groups[1]:
        if step != (0, 0):
            pl.semaphore_signal(barrier, inc=1, device_id=device(ahead(step)), device_id_type=MESH)
    pl.semaphore_wait(barrier, chips)

    recvs = (recv_a, recv_b)

    def dispatch(g, q):
        step = groups[g][q]
        n = g * half + q
        dst = recvs[g].at[pl.ds(q * size, size)]
        if step == (0, 0):
            return pltpu.make_async_copy(send_ref.at[chip], dst, in_sem.at[n])
        to = ahead(step)
        return pltpu.make_async_remote_copy(
            src_ref=send_ref.at[to], dst_ref=dst, send_sem=out_sem.at[n], recv_sem=in_sem.at[n],
            device_id=device(to), device_id_type=MESH)

    def swap(k, j):
        src, dst = ((w1o, w1p), (w2o, w2p))[k]
        return pltpu.make_async_remote_copy(
            src_ref=src.at[j], dst_ref=dst.at[j], send_sem=swap_out_sem.at[k, j], recv_sem=swap_in_sem.at[k, j],
            device_id=partner, device_id_type=MESH)

    def give(g, q):
        step = groups[g][q]
        n = g * half + q
        src = ret_v.at[n]
        if step == (0, 0):
            return pltpu.make_async_copy(src, back_ref.at[chip], ret_in_sem.at[n])
        return pltpu.make_async_remote_copy(
            src_ref=src, dst_ref=back_ref.at[chip], send_sem=ret_out_sem.at[n], recv_sem=ret_in_sem.at[n],
            device_id=device(behind(step)), device_id_type=MESH)

    def dispatch_start(g, late):
        for q in range(half):
            if (groups[g][q][1] == 0) == late:
                dispatch(g, q).start()

    def dispatch_end(g, q):
        if groups[g][q] == (0, 0):
            dispatch(g, q).wait()
        else:
            dispatch(g, q).wait_recv()

    dispatch_start(0, False)

    def swap_start(j, c):
        swap(0, j).start()
        swap(1, j).start()
        return c
    lax.fori_loop(0, exp_dev, swap_start, 0)

    def load(a, b, j, slot):
        return (pltpu.make_async_copy(a.at[j], w1_v.at[slot], w_sem.at[0, slot]),
                pltpu.make_async_copy(b.at[j], w2_v.at[slot], w_sem.at[1, slot]))

    def load_start(a, b, j, slot):
        for d in load(a, b, j, slot):
            d.start()

    def load_wait(slot):
        for d in load(w1o, w2o, 0, slot):
            d.wait()

    def compute(g, i, slot):
        recv = recvs[g]
        for q in range(half):
            a = start_ref[i, behind(groups[g][q])] + q * size
            v = jnp.stack([recv[a + j] for j in range(cap_slot)]).astype(F32)
            x2[pl.ds(q * cap_slot, cap_slot), :] = v.reshape(cap_slot, SUB * LANE).astype(BF16)
        h = jnp.dot(x2[...], w1_v[slot], preferred_element_type=F32)
        h = jax.nn.gelu(h, approximate=True).astype(BF16)
        z = jnp.dot(h, w2_v[slot], preferred_element_type=F32).astype(BF16).astype(F32)
        rows = half * cap_slot
        ze[pl.ds(pl.multiple_of(i * rows, rows), rows)] = z.reshape(rows, SUB, LANE).astype(BF16)

    for g in range(2):
        load_start(w1o, w2o, 0, 0)
        early = [q for q in range(half) if groups[g][q][1] != 0]
        if g == 0:
            for q in early[:half // 2]:
                dispatch_end(g, q)
            dispatch_start(0, True)
            dispatch_start(1, False)
            early = early[half // 2:]
        for q in early + [q for q in range(half) if groups[g][q][1] == 0]:
            dispatch_end(g, q)

        def own(j, c):
            slot = j % 2

            @pl.when(j + 1 < exp_dev)
            def _():
                load_start(w1o, w2o, j + 1, 1 - slot)
            load_wait(slot)
            compute(g, core * exp_dev + j, slot)
            return c
        lax.fori_loop(0, exp_dev, own, 0)
        if g == 0:
            dispatch_start(1, True)

        def ready(j):
            if g == 0:
                swap(0, j).wait_recv()
                swap(1, j).wait_recv()
        ready(0)
        load_start(w1p, w2p, 0, 0)

        def theirs(j, c):
            slot = j % 2

            @pl.when(j + 1 < exp_dev)
            def _():
                ready(j + 1)
                load_start(w1p, w2p, j + 1, 1 - slot)
            load_wait(slot)
            compute(g, (1 - core) * exp_dev + j, slot)
            return c
        lax.fori_loop(0, exp_dev, theirs, 0)

        for q in range(half):
            lane = behind(groups[g][q])
            n = g * half + q

            def rows(b, c):
                for u in range(unroll(size)):
                    r = b * unroll(size) + u
                    ret_v[n, r] = ze[map_ref[lane, r] + q * cap_slot]
                return c
            lax.fori_loop(0, size // unroll(size), rows, 0)
            if q > 0:
                give(g, q - 1).start()
        give(g, half - 1).start()

    def swap_end(j, c):
        swap(0, j).wait_send()
        swap(1, j).wait_send()
        return c
    lax.fori_loop(0, exp_dev, swap_end, 0)
    for g in range(2):
        for q in range(half):
            if groups[g][q] == (0, 0):
                give(g, q).wait()
            else:
                dispatch(g, q).wait_send()
                give(g, q).wait()


def ffn_kernel(size, cap_slot, start_ref, cnt_ref, core_ref, recv_ref, w1o, w1p, w2o, w2p, out_ref,
               recv_v, ret_v, w1_v, w2_v, xe, ze, x2, recv_sem, w_sem, out_sem):
    srcs = recv_ref.shape[0]
    exp_dev = w1o.shape[0]
    exp_chip = CORES * exp_dev
    core = core_ref[0]
    block = x2.shape[0]

    def recv_copy(s):
        return pltpu.make_async_copy(recv_ref.at[s], recv_v.at[pl.ds(s * size, size)], recv_sem.at[s])

    def out_copy(s):
        return pltpu.make_async_copy(ret_v.at[s, pl.ds(0, size)], out_ref.at[s], out_sem.at[s])

    def w_start(i):
        slot = i % 2
        local = i % exp_dev

        @pl.when(i // exp_dev == core)
        def _():
            pltpu.make_async_copy(w1o.at[local], w1_v.at[slot], w_sem.at[0, slot]).start()
            pltpu.make_async_copy(w2o.at[local], w2_v.at[slot], w_sem.at[1, slot]).start()

        @pl.when(i // exp_dev != core)
        def _():
            pltpu.make_async_copy(w1p.at[local], w1_v.at[slot], w_sem.at[0, slot]).start()
            pltpu.make_async_copy(w2p.at[local], w2_v.at[slot], w_sem.at[1, slot]).start()

    def w_wait(i):
        slot = i % 2
        pltpu.make_async_copy(w1o.at[0], w1_v.at[slot], w_sem.at[0, slot]).wait()
        pltpu.make_async_copy(w2o.at[0], w2_v.at[slot], w_sem.at[1, slot]).wait()

    for s in range(srcs):
        recv_copy(s).start()
    w_start(jnp.int32(0))
    for s in range(srcs):
        recv_copy(s).wait()

    def expert(i, c):
        slot = i % 2

        @pl.when(i + 1 < exp_chip)
        def _():
            w_start(i + 1)

        def gather(s, pos):
            n = cnt_ref[i, s]

            @pl.when(n > 0)
            def _():
                a = s * size + start_ref[i, s]
                for j in range(cap_slot):
                    xe[pos + j] = recv_v[a + j]
            return pos + n
        total = lax.fori_loop(0, srcs, gather, jnp.int32(0))
        w_wait(i)

        def tile(b, c2):
            base = pl.multiple_of(b * block, block)
            for q in range(block // 16):
                v = xe[pl.ds(base + q * 16, 16)].astype(F32).reshape(16, SUB * LANE)
                x2[pl.ds(q * 16, 16), :] = v.astype(BF16)
            h = jnp.dot(x2[...], w1_v[slot], preferred_element_type=F32)
            h = jax.nn.gelu(h, approximate=True).astype(BF16)
            z = jnp.dot(h, w2_v[slot], preferred_element_type=F32).astype(BF16).astype(F32)
            ze[pl.ds(base, block)] = z.reshape(block, SUB, LANE).astype(BF16)
            return c2
        lax.fori_loop(0, (total + block - 1) // block, tile, 0)

        def scatter(s, pos):
            n = cnt_ref[i, s]

            @pl.when(n > 0)
            def _():
                a = start_ref[i, s]
                for j in range(cap_slot):
                    ret_v[s, a + j] = ze[pos + j]
            return pos + n
        lax.fori_loop(0, srcs, scatter, jnp.int32(0))
        return c
    lax.fori_loop(0, exp_chip, expert, 0)
    for s in range(srcs):
        out_copy(s).start()
    for s in range(srcs):
        out_copy(s).wait()


def combine_kernel(row_ref, gate_ref, x_ref, ret_ref, out_ref, ret_v, x_v, out_v, y3, sem, x_sem, out_sem):
    tokens, d_model = x_ref.shape
    lanes, size = ret_ref.shape[:2]
    last = lanes * size - 1
    block = 16
    parts = x_sem.shape[0]
    part = tokens // parts

    def copy(s):
        return pltpu.make_async_copy(ret_ref.at[s], ret_v.at[pl.ds(s * size, size)], sem.at[s])

    def x_copy(p):
        rows = pl.ds(p * part, part)
        return pltpu.make_async_copy(x_ref.at[rows], x_v.at[rows], x_sem.at[p])

    def out_copy(p):
        rows = pl.ds(p * part, part)
        return pltpu.make_async_copy(out_v.at[rows], out_ref.at[rows], out_sem.at[p])
    for s in range(lanes):
        copy(s).start()
    for p in range(parts):
        x_copy(p).start()
    for s in range(lanes):
        copy(s).wait()

    def step(i, c):
        base = pl.multiple_of(i * block, block)
        for u in range(block):
            t = base + u
            g1 = gate_ref[0, t]
            g2 = gate_ref[1, t]
            z1 = ret_v[jnp.minimum(row_ref[0, t], last)].astype(F32)
            z2 = ret_v[jnp.minimum(row_ref[1, t], last)].astype(F32)
            y3[u] = jnp.where(g1 > 0, g1 * z1, 0.0) + jnp.where(g2 > 0, g2 * z2, 0.0)
        r = pl.ds(base, block)
        y = y3[...].reshape(block, d_model)
        out_v[r, :] = (x_v[r, :].astype(F32) + y).astype(BF16)
        return c
    for p in range(parts):
        x_copy(p).wait()
        lax.fori_loop(p * part // block, (p + 1) * part // block, step, 0)
        out_copy(p).start()
    for p in range(parts):
        out_copy(p).wait()


def spec(space):
    return pl.BlockSpec(memory_space=space)


SMEM = pltpu.SMEM
VMEM = pltpu.VMEM
ANY = pl.ANY


def params(number=None):
    if number is None:
        return pltpu.CompilerParams(vmem_limit_bytes=VMEM_LIMIT)
    return pltpu.CompilerParams(vmem_limit_bytes=VMEM_LIMIT, collective_id=number, has_side_effects=True)


def solution(mesh):
    devs = mesh.shape['ep']
    row_spec = P(('dp', 'ep'), None)
    expert_spec = P('ep', None, None)
    classes = [[i for i in range(devs) if i % CORES == c] for c in range(CORES)]
    partner = [(i, i ^ 1) for i in range(devs)]
    dma = pltpu.SemaphoreType.DMA

    def local_step(x_rows, logits, w_in, w_out):
        tokens, d_model = x_rows.shape
        experts = logits.shape[1]
        exp_dev, _, hidden = w_in.shape
        capacity = CAP_FACTOR * tokens * devs // experts
        cap_slot = capslot(tokens, experts)
        exp_chip = CORES * exp_dev
        chips = devs // CORES
        half = chips // 2
        full = exp_chip * cap_slot
        sizes = tuple(full * k // 32 for k in (21, 23, 32))
        core = (lax.axis_index('ep').astype(I32) % CORES).reshape(1)

        row, keep, start, cnt, back_map, pick = pl.pallas_call(
            functools.partial(route_kernel, sizes, capacity, exp_dev), name='route',
            out_shape=(jax.ShapeDtypeStruct((8, tokens), I32), jax.ShapeDtypeStruct((8, tokens), F32),
                       jax.ShapeDtypeStruct((exp_chip, chips), I32), jax.ShapeDtypeStruct((exp_chip, chips), I32),
                       jax.ShapeDtypeStruct((chips, full), I32), jax.ShapeDtypeStruct((8, LANE), I32)),
            in_specs=[spec(VMEM)],
            scratch_shapes=[VMEM((8, experts), F32), VMEM((devs, 8, experts), F32), dma((devs,)), dma((devs,))],
            compiler_params=params(0))(logits)

        def pack(size, row, x_rows):
            return pl.pallas_call(
                functools.partial(send_kernel, size), name='send',
                out_shape=jax.ShapeDtypeStruct((chips, size, SUB, LANE), BF16),
                in_specs=[spec(SMEM), spec(ANY)], out_specs=spec(ANY),
                scratch_shapes=[SMEM((chips * size + 8,), I32), VMEM((tokens, d_model), BF16),
                                VMEM((tokens, SUB, LANE), BF16), VMEM((4, size, SUB, LANE), BF16),
                                dma((4,)), dma((4,))],
                compiler_params=params())(row, x_rows)

        def combine(size, row, keep, x_rows, back):
            return pl.pallas_call(
                combine_kernel, name='combine', out_shape=jax.ShapeDtypeStruct((tokens, d_model), BF16),
                in_specs=[spec(SMEM)] * 2 + [spec(ANY)] * 2, out_specs=spec(ANY),
                scratch_shapes=[VMEM((chips * size, SUB, LANE), BF16), VMEM((tokens, d_model), BF16),
                                VMEM((tokens, d_model), BF16), VMEM((16, SUB, LANE), F32),
                                dma((chips,)), dma((4,)), dma((4,))],
                compiler_params=params())(row, keep, x_rows, back)

        def fused(number, size, x_rows, w_in, w_out, row, keep, start, cnt, back_map):
            lane_shape = jax.ShapeDtypeStruct((chips, size, SUB, LANE), BF16)
            send = pack(size, row, x_rows)
            back, _, _ = pl.pallas_call(
                functools.partial(moe_kernel, size, cap_slot), name='moe',
                out_shape=(lane_shape, jax.ShapeDtypeStruct(w_in.shape, BF16),
                           jax.ShapeDtypeStruct(w_out.shape, BF16)),
                in_specs=[spec(SMEM)] * 2 + [spec(ANY)] * 3, out_specs=(spec(ANY),) * 3,
                scratch_shapes=[
                    VMEM((half * size + cap_slot, SUB, LANE), BF16),
                    VMEM((half * size + cap_slot, SUB, LANE), BF16),
                    VMEM((chips, size, SUB, LANE), BF16),
                    VMEM((exp_chip * half * cap_slot, SUB, LANE), BF16),
                    VMEM((2, d_model, hidden), BF16), VMEM((2, hidden, d_model), BF16),
                    VMEM((half * cap_slot, d_model), BF16),
                    dma((chips,)), dma((chips,)), dma((chips,)), dma((chips,)),
                    dma((2, exp_dev)), dma((2, exp_dev)), dma((2, 2))],
                compiler_params=params(number))(start, back_map, send, w_in, w_out)
            return combine(size, row, keep, x_rows, back)

        def general(size, x_rows, w_in, w_out, row, keep, start, cnt, back_map):
            w_in_p = lax.ppermute(w_in, 'ep', partner)
            w_out_p = lax.ppermute(w_out, 'ep', partner)
            send = pack(size, row, x_rows)
            recv = lax.all_to_all(send, 'ep', 0, 0, axis_index_groups=classes, tiled=True)
            rows_max = capacity + cap_slot
            ret = pl.pallas_call(
                functools.partial(ffn_kernel, size, cap_slot), name='ffn',
                out_shape=jax.ShapeDtypeStruct((chips, size, SUB, LANE), BF16),
                in_specs=[spec(SMEM)] * 3 + [spec(ANY)] * 5, out_specs=spec(ANY),
                scratch_shapes=[
                    VMEM((chips * size + cap_slot, SUB, LANE), BF16),
                    VMEM((chips, size + cap_slot, SUB, LANE), BF16),
                    VMEM((2, d_model, hidden), BF16), VMEM((2, hidden, d_model), BF16),
                    VMEM((rows_max, SUB, LANE), BF16), VMEM((rows_max, SUB, LANE), BF16),
                    VMEM((LANE, d_model), BF16), dma((chips,)), dma((2, 2)), dma((chips,))],
                compiler_params=params())(start, cnt, core, recv, w_in, w_in_p, w_out, w_out_p)
            back = lax.all_to_all(ret, 'ep', 0, 0, axis_index_groups=classes, tiled=True)
            return combine(size, row, keep, x_rows, back)

        branches = [functools.partial(fused, 1 + k, size) for k, size in enumerate(sizes[:-1])]
        branches.append(functools.partial(general, sizes[-1]))
        return lax.switch(pick[0, 0], branches, x_rows, w_in, w_out, row, keep, start, cnt, back_map)

    return jax.shard_map(local_step, mesh=mesh, in_specs=(row_spec, row_spec, expert_spec, expert_spec),
                         out_specs=row_spec, check_vma=False)
```

```python
import functools

import jax
import jax.numpy as jnp
from jax import lax
from jax.experimental import pallas as pl
from jax.experimental.pallas import tpu as pltpu
from jax.sharding import PartitionSpec as P

CAP_FACTOR = 2
SLOT_FACTOR = 4
CORES = 2
SUB = 16
WEIGHT_SLOTS = 6
LANE = 128
VMEM_LIMIT = 62 * 1024 * 1024
BF16 = jnp.bfloat16
F32 = jnp.float32
I32 = jnp.int32


MESH = pl.DeviceIdType.MESH


def iota(shape, dim):
    return lax.broadcasted_iota(I32, shape, dim)


def route_kernel(sizes, capacity, exp_dev, logits_ref, row_ref, keep_ref, start_ref, cnt_ref, back_ref, pick_ref,
                 stage, counts_v, send_sem, recv_sem):
    tokens, experts = logits_ref.shape
    devs = counts_v.shape[0]
    exp_chip = CORES * exp_dev
    me = lax.axis_index('ep')
    chip = me // CORES
    core = me % CORES
    barrier = pltpu.get_barrier_semaphore()

    def other(d):
        return {'ep': (me + d) % devs}

    def hello(d, c):
        pl.semaphore_signal(barrier, inc=1, device_id=other(d), device_id_type=MESH)
        return c
    lax.fori_loop(1, devs, hello, 0)

    lt = logits_ref[...].T
    ids = iota(lt.shape, 0)
    m1 = jnp.max(lt, axis=0, keepdims=True)
    e1 = jnp.min(jnp.where(lt == m1, ids, experts), axis=0, keepdims=True)
    rest = jnp.where(ids == e1, -jnp.inf, lt)
    m2 = jnp.max(rest, axis=0, keepdims=True)
    e2 = jnp.min(jnp.where(rest == m2, ids, experts), axis=0, keepdims=True)
    hit1 = ids == e1
    hit2 = ids == e2
    chosen = jnp.where(hit1 | hit2, 1.0, 0.0).astype(BF16)
    ones = jnp.ones((8, tokens), BF16)
    count = lax.dot_general(ones, chosen, (((1,), (1,)), ((), ())), preferred_element_type=F32)
    stage[...] = count
    counts_v[me] = count
    pl.semaphore_wait(barrier, devs - 1)

    def copy(d):
        return pltpu.make_async_remote_copy(
            src_ref=stage, dst_ref=counts_v.at[me], send_sem=send_sem.at[d], recv_sem=recv_sem.at[d],
            device_id=other(d), device_id_type=MESH)

    def start_copy(d, c):
        copy(d).start()
        return c

    total = jnp.sum(jnp.exp(lt - m1), axis=0, keepdims=True)
    gates = (1.0 / total, jnp.exp(m2 - m1) / total)
    lax.fori_loop(1, devs, start_copy, 0)
    upper = jnp.where(iota((tokens, tokens), 0) < iota((tokens, tokens), 1), 1.0, 0.0).astype(BF16)
    before = jnp.dot(chosen, upper, preferred_element_type=F32)
    pos1 = jnp.sum(jnp.where(hit1, before, 0.0), axis=0, keepdims=True).astype(I32)
    pos2 = jnp.sum(jnp.where(hit2, before, 0.0), axis=0, keepdims=True).astype(I32)

    def wait_copy(d, c):
        copy(d).wait()
        return c
    lax.fori_loop(1, devs, wait_copy, 0)

    counts = counts_v[:, 0, :]
    lower = jnp.where(iota((devs, devs), 1) < iota((devs, devs), 0), 1.0, 0.0).astype(BF16)
    offs = jnp.dot(lower, counts.astype(BF16), preferred_element_type=F32)
    kept = jnp.minimum(jnp.maximum(capacity - offs, 0.0), counts)
    kept_b = kept.astype(BF16)
    row_e = iota((experts, experts), 0)
    col_e = iota((experts, experts), 1)
    same = (row_e // exp_chip == col_e // exp_chip) & (row_e < col_e)
    start = jnp.dot(kept_b, jnp.where(same, 1.0, 0.0).astype(BF16), preferred_element_type=F32)
    start_b = start.astype(BF16)
    member = jnp.where(iota((experts, LANE), 0) // exp_chip == iota((experts, LANE), 1), 1.0, 0.0).astype(BF16)
    totals = jnp.dot(kept_b, member, preferred_element_type=F32)
    most = jnp.max(jnp.max(totals, axis=0, keepdims=True), axis=1, keepdims=True).astype(I32)
    size = jnp.full((1, 1), sizes[0], I32)
    pick = jnp.zeros((1, 1), I32)
    for small, large in zip(sizes[:-1], sizes[1:]):
        size = jnp.where(most > small, large, size)
        pick = pick + jnp.where(most > small, 1, 0)
    pick_ref[...] = jnp.broadcast_to(pick, pick_ref.shape)

    mine = iota((devs, experts), 0) == me
    my_start = jnp.sum(jnp.where(mine, start, 0.0), axis=0, keepdims=True)
    my_kept = jnp.sum(jnp.where(mine, kept, 0.0), axis=0, keepdims=True)
    look = jnp.concatenate([my_start, my_kept, jnp.zeros((6, experts), F32)], axis=0).astype(BF16)
    lanes = experts // exp_chip
    for k, (e, hit, pos) in enumerate(((e1, hit1, pos1), (e2, hit2, pos2))):
        got = jnp.dot(look, jnp.where(hit, 1.0, 0.0).astype(BF16), preferred_element_type=F32).astype(I32)
        keep = pos < got[1:2, :]
        row = (e // exp_chip) * size + got[0:1, :] + pos
        row_ref[k:k + 1, :] = jnp.where(keep, row, lanes * size)
        keep_ref[k:k + 1, :] = jnp.where(keep, gates[k], 0.0)

    srcs = devs // CORES
    pick_src = jnp.where(iota((srcs, devs), 1) == CORES * iota((srcs, devs), 0) + core, 1.0, 0.0).astype(BF16)
    pick_exp = jnp.where(iota((exp_chip, experts), 1) == chip * exp_chip + iota((exp_chip, experts), 0),
                         1.0, 0.0).astype(BF16)
    contract = (((1,), (1,)), ((), ()))

    def mine_of(table):
        part = lax.dot_general(pick_exp, table, contract, preferred_element_type=F32).astype(BF16)
        return lax.dot_general(part, pick_src, contract, preferred_element_type=F32).astype(I32)
    first = mine_of(start_b)
    count = mine_of(kept_b)
    start_ref[...] = first
    cnt_ref[...] = count
    width = back_ref.shape[1]
    ids = iota((exp_chip, width), 0)
    rows = iota((exp_chip, width), 1)
    group_rows = (srcs // 2) * capslot(tokens, experts)
    for s in range(srcs):
        off = rows - first[:, s:s + 1]
        inside = (off >= 0) & (off < count[:, s:s + 1])
        back_ref[s:s + 1, :] = jnp.sum(jnp.where(inside, ids * group_rows + off, 0), axis=0, keepdims=True)


def unroll(size):
    return max(k for k in range(1, 49) if size % k == 0)


def send_kernel(size, row_ref, x_ref, out_ref, tok, x_v, rows3, stage, x_sem, sem):
    tokens, d_model = x_ref.shape
    lanes = out_ref.shape[0]
    block = 16
    parts = x_sem.shape[0]
    part = tokens // parts

    def x_copy(p):
        rows = pl.ds(p * part, part)
        return pltpu.make_async_copy(x_ref.at[rows], x_v.at[rows], x_sem.at[p])
    for p in range(parts):
        x_copy(p).start()

    def fill(i, c):
        for u in range(16):
            t = i * 16 + u
            tok[row_ref[0, t]] = t
            tok[row_ref[1, t]] = t
        return c
    lax.fori_loop(0, tokens // 16, fill, 0)

    def relayout(i, c):
        r = pl.ds(pl.multiple_of(i * block, block), block)
        rows3[r] = x_v[r].astype(F32).reshape(block, SUB, LANE).astype(BF16)
        return c
    for p in range(parts):
        x_copy(p).wait()
        lax.fori_loop(p * part // block, (p + 1) * part // block, relayout, 0)

    slots = stage.shape[0]
    step = unroll(size)

    def copy(lane, slot):
        return pltpu.make_async_copy(stage.at[slot], out_ref.at[lane], sem.at[slot])

    def lane_step(lane, c):
        slot = lane % slots

        @pl.when(lane >= slots)
        def _():
            copy(lane - slots, slot).wait()

        def rows(i, c2):
            for u in range(step):
                r = i * step + u
                t = tok[lane * size + r]
                t = t & (tokens - 1) if tokens & (tokens - 1) == 0 else jnp.clip(t, 0, tokens - 1)
                stage[slot, r] = rows3[t]
            return c2
        lax.fori_loop(0, size // step, rows, 0)
        copy(lane, slot).start()
        return c
    lax.fori_loop(0, lanes, lane_step, 0)
    for k in range(min(slots, lanes)):
        lane = lanes - min(slots, lanes) + k
        copy(lane, lane % slots).wait()


def capslot(tokens, experts):
    return SLOT_FACTOR * tokens // experts


def grid_side(chips):
    return max(k for k in range(1, chips + 1) if chips % k == 0 and k * k <= chips)


def shifts_of(chips):
    side = grid_side(chips)
    tall = chips // side
    steps = [(dy, dx) for dy in range(tall) for dx in range(side)]
    near = [s for s in steps if s != (0, 0) and 2 * s[0] != tall and 2 * s[1] != side]
    if 2 * len(near) != chips:
        near = [s for s in steps if (s[0] + s[1]) % 2 == 0]
    far = [s for s in steps if s not in near]
    turn = (tall - 1) * (side - 1) + 1

    def rank(s):
        return (0 in s, s == (0, 0), s[1] == 0, (s[0] * turn + s[1]) % 2, s[0] != s[1])
    return sorted(near, key=rank), sorted(far, key=rank)


def moe_kernel(size, cap_slot, start_ref, map_ref, send_ref, w1o, w2o, back_ref, w1p, w2p,
               recv_a, recv_b, ret_v, ze, w1_v, w2_v, x2,
               out_sem, in_sem, ret_out_sem, ret_in_sem, swap_out_sem, swap_in_sem, w_sem):
    chips = send_ref.shape[0]
    exp_dev = w1o.shape[0]
    exp_chip = CORES * exp_dev
    groups = shifts_of(chips)
    half = len(groups[0])
    side = grid_side(chips)
    tall = chips // side
    me = lax.axis_index('ep')
    chip = me // CORES
    core = me % CORES
    cy = chip // side
    cx = chip % side
    partner = {'ep': chip * CORES + (1 - core)}

    def ahead(step):
        return ((cy + step[0]) % tall) * side + (cx + step[1]) % side

    def behind(step):
        return ((cy + tall - step[0]) % tall) * side + (cx + side - step[1]) % side

    def device(c):
        return {'ep': c * CORES + core}

    barrier = pltpu.get_barrier_semaphore()
    pl.semaphore_signal(barrier, inc=1, device_id=partner, device_id_type=MESH)
    for step in groups[0] + groups[1]:
        if step != (0, 0):
            pl.semaphore_signal(barrier, inc=1, device_id=device(ahead(step)), device_id_type=MESH)
    pl.semaphore_wait(barrier, chips)

    recvs = (recv_a, recv_b)

    def dispatch(g, q):
        step = groups[g][q]
        n = g * half + q
        dst = recvs[g].at[pl.ds(q * size, size)]
        if step == (0, 0):
            return pltpu.make_async_copy(send_ref.at[chip], dst, in_sem.at[n])
        to = ahead(step)
        return pltpu.make_async_remote_copy(
            src_ref=send_ref.at[to], dst_ref=dst, send_sem=out_sem.at[n], recv_sem=in_sem.at[n],
            device_id=device(to), device_id_type=MESH)

    def swap(k, j):
        src, dst = ((w1o, w1p), (w2o, w2p))[k]
        return pltpu.make_async_remote_copy(
            src_ref=src.at[j], dst_ref=dst.at[j], send_sem=swap_out_sem.at[k, j], recv_sem=swap_in_sem.at[k, j],
            device_id=partner, device_id_type=MESH)

    def give(g, q):
        step = groups[g][q]
        n = g * half + q
        src = ret_v.at[n]
        if step == (0, 0):
            return pltpu.make_async_copy(src, back_ref.at[chip], ret_in_sem.at[n])
        return pltpu.make_async_remote_copy(
            src_ref=src, dst_ref=back_ref.at[chip], send_sem=ret_out_sem.at[n], recv_sem=ret_in_sem.at[n],
            device_id=device(behind(step)), device_id_type=MESH)

    def dispatch_start(g, late):
        for q in range(half):
            if (groups[g][q][1] == 0) == late:
                dispatch(g, q).start()

    def dispatch_end(g, q):
        if groups[g][q] == (0, 0):
            dispatch(g, q).wait()
        else:
            dispatch(g, q).wait_recv()

    dispatch_start(0, False)

    def swap_start(j, c):
        swap(0, j).start()
        swap(1, j).start()
        return c
    lax.fori_loop(0, exp_dev, swap_start, 0)

    slots = w1_v.shape[0]

    def load(a, b, j, slot):
        return (pltpu.make_async_copy(a.at[j], w1_v.at[slot], w_sem.at[0, slot]),
                pltpu.make_async_copy(b.at[j], w2_v.at[slot], w_sem.at[1, slot]))

    def load_start(p, slot, first):
        @pl.when(p < exp_dev)
        def _():
            for d in load(w1o, w2o, p, slot):
                d.start()

        @pl.when(p >= exp_dev)
        def _():
            j = p - exp_dev
            if first:
                swap(0, j).wait_recv()
                swap(1, j).wait_recv()
            for d in load(w1p, w2p, j, slot):
                d.start()

    def load_wait(slot):
        for d in load(w1o, w2o, 0, slot):
            d.wait()

    def compute(g, i, slot):
        recv = recvs[g]
        for q in range(half):
            a = start_ref[i, behind(groups[g][q])] + q * size
            v = jnp.stack([recv[a + j] for j in range(cap_slot)]).astype(F32)
            x2[pl.ds(q * cap_slot, cap_slot), :] = v.reshape(cap_slot, SUB * LANE).astype(BF16)
        h = jnp.dot(x2[...], w1_v[slot], preferred_element_type=F32)
        h = jax.nn.gelu(h, approximate=True).astype(BF16)
        z = jnp.dot(h, w2_v[slot], preferred_element_type=F32).astype(BF16).astype(F32)
        rows = half * cap_slot
        ze[pl.ds(pl.multiple_of(i * rows, rows), rows)] = z.reshape(rows, SUB, LANE).astype(BF16)

    def is_late(g, q):
        return groups[g][q][1] == 0

    def pack_back(g):
        for q in range(half):
            lane = behind(groups[g][q])
            n = g * half + q

            def rows(b, c):
                for u in range(unroll(size)):
                    r = b * unroll(size) + u
                    ret_v[n, r] = ze[map_ref[lane, r] + q * cap_slot]
                return c
            lax.fori_loop(0, size // unroll(size), rows, 0)
            if q > 0 and not is_late(g, q - 1):
                give(g, q - 1).start()
        if not is_late(g, half - 1):
            give(g, half - 1).start()

    def give_late(g):
        for q in range(half):
            if is_late(g, q):
                give(g, q).start()

    depth = slots - 1
    for p in range(depth):
        for d in load(w1o, w2o, p, p):
            d.start()
    early = [q for q in range(half) if not is_late(0, q)]
    late = [q for q in range(half) if is_late(0, q)]
    for q in early[:half // 2]:
        dispatch_end(0, q)
    dispatch_start(0, True)
    dispatch_start(1, False)
    for q in early[half // 2:] + late:
        dispatch_end(0, q)

    def first_pass(p, c):
        @pl.when(p + depth < exp_chip)
        def _():
            load_start(p + depth, (p + depth) % slots, True)

        @pl.when(p == exp_dev)
        def _():
            dispatch_start(1, True)
        slot = p % slots
        load_wait(slot)
        compute(0, (core * exp_dev + p) % exp_chip, slot)
        return c
    lax.fori_loop(0, exp_chip, first_pass, 0)
    pack_back(0)
    for q in range(half):
        dispatch_end(1, q)
    give_late(0)
    held = exp_chip - slots

    def second_pass(b, c):
        slot = (held + b) % slots

        @pl.when(b >= slots)
        def _():
            load_wait(slot)
        compute(1, (core * exp_dev + held + b) % exp_chip, slot)

        @pl.when(b < held)
        def _():
            load_start(b, slot, False)
        return c
    lax.fori_loop(0, exp_chip, second_pass, 0)
    pack_back(1)
    for q in range(half):
        give(0, q).wait_recv() if groups[0][q] != (0, 0) else give(0, q).wait()
    give_late(1)

    def swap_end(j, c):
        swap(0, j).wait_send()
        swap(1, j).wait_send()
        return c
    lax.fori_loop(0, exp_dev, swap_end, 0)
    for g in range(2):
        for q in range(half):
            if groups[g][q] != (0, 0):
                dispatch(g, q).wait_send()
                give(g, q).wait_send()
            if g == 1:
                give(g, q).wait() if groups[g][q] == (0, 0) else give(g, q).wait_recv()


def ffn_kernel(size, cap_slot, start_ref, cnt_ref, core_ref, recv_ref, w1o, w1p, w2o, w2p, out_ref,
               recv_v, ret_v, w1_v, w2_v, xe, ze, x2, recv_sem, w_sem, out_sem):
    srcs = recv_ref.shape[0]
    exp_dev = w1o.shape[0]
    exp_chip = CORES * exp_dev
    core = core_ref[0]
    block = x2.shape[0]

    def recv_copy(s):
        return pltpu.make_async_copy(recv_ref.at[s], recv_v.at[pl.ds(s * size, size)], recv_sem.at[s])

    def out_copy(s):
        return pltpu.make_async_copy(ret_v.at[s, pl.ds(0, size)], out_ref.at[s], out_sem.at[s])

    def w_start(i):
        slot = i % 2
        local = i % exp_dev

        @pl.when(i // exp_dev == core)
        def _():
            pltpu.make_async_copy(w1o.at[local], w1_v.at[slot], w_sem.at[0, slot]).start()
            pltpu.make_async_copy(w2o.at[local], w2_v.at[slot], w_sem.at[1, slot]).start()

        @pl.when(i // exp_dev != core)
        def _():
            pltpu.make_async_copy(w1p.at[local], w1_v.at[slot], w_sem.at[0, slot]).start()
            pltpu.make_async_copy(w2p.at[local], w2_v.at[slot], w_sem.at[1, slot]).start()

    def w_wait(i):
        slot = i % 2
        pltpu.make_async_copy(w1o.at[0], w1_v.at[slot], w_sem.at[0, slot]).wait()
        pltpu.make_async_copy(w2o.at[0], w2_v.at[slot], w_sem.at[1, slot]).wait()

    for s in range(srcs):
        recv_copy(s).start()
    w_start(jnp.int32(0))
    for s in range(srcs):
        recv_copy(s).wait()

    def expert(i, c):
        slot = i % 2

        @pl.when(i + 1 < exp_chip)
        def _():
            w_start(i + 1)

        def gather(s, pos):
            n = cnt_ref[i, s]

            @pl.when(n > 0)
            def _():
                a = s * size + start_ref[i, s]
                for j in range(cap_slot):
                    xe[pos + j] = recv_v[a + j]
            return pos + n
        total = lax.fori_loop(0, srcs, gather, jnp.int32(0))
        w_wait(i)

        def tile(b, c2):
            base = pl.multiple_of(b * block, block)
            for q in range(block // 16):
                v = xe[pl.ds(base + q * 16, 16)].astype(F32).reshape(16, SUB * LANE)
                x2[pl.ds(q * 16, 16), :] = v.astype(BF16)
            h = jnp.dot(x2[...], w1_v[slot], preferred_element_type=F32)
            h = jax.nn.gelu(h, approximate=True).astype(BF16)
            z = jnp.dot(h, w2_v[slot], preferred_element_type=F32).astype(BF16).astype(F32)
            ze[pl.ds(base, block)] = z.reshape(block, SUB, LANE).astype(BF16)
            return c2
        lax.fori_loop(0, (total + block - 1) // block, tile, 0)

        def scatter(s, pos):
            n = cnt_ref[i, s]

            @pl.when(n > 0)
            def _():
                a = start_ref[i, s]
                for j in range(cap_slot):
                    ret_v[s, a + j] = ze[pos + j]
            return pos + n
        lax.fori_loop(0, srcs, scatter, jnp.int32(0))
        return c
    lax.fori_loop(0, exp_chip, expert, 0)
    for s in range(srcs):
        out_copy(s).start()
    for s in range(srcs):
        out_copy(s).wait()


def combine_kernel(row_ref, gate_ref, x_ref, ret_ref, out_ref, ret_v, x_v, out_v, y3, sem, x_sem, out_sem):
    tokens, d_model = x_ref.shape
    lanes, size = ret_ref.shape[:2]
    last = lanes * size - 1
    block = 16
    parts = x_sem.shape[0]
    part = tokens // parts

    def copy(s):
        return pltpu.make_async_copy(ret_ref.at[s], ret_v.at[pl.ds(s * size, size)], sem.at[s])

    def x_copy(p):
        rows = pl.ds(p * part, part)
        return pltpu.make_async_copy(x_ref.at[rows], x_v.at[rows], x_sem.at[p])

    def out_copy(p):
        rows = pl.ds(p * part, part)
        return pltpu.make_async_copy(out_v.at[rows], out_ref.at[rows], out_sem.at[p])
    for s in range(lanes):
        copy(s).start()
    for p in range(parts):
        x_copy(p).start()
    for s in range(lanes):
        copy(s).wait()

    def step(i, c):
        base = pl.multiple_of(i * block, block)
        for u in range(block):
            t = base + u
            g1 = gate_ref[0, t]
            g2 = gate_ref[1, t]
            z1 = ret_v[jnp.minimum(row_ref[0, t], last)].astype(F32)
            z2 = ret_v[jnp.minimum(row_ref[1, t], last)].astype(F32)
            y3[u] = jnp.where(g1 > 0, g1 * z1, 0.0) + jnp.where(g2 > 0, g2 * z2, 0.0)
        r = pl.ds(base, block)
        y = y3[...].reshape(block, d_model)
        out_v[r, :] = (x_v[r, :].astype(F32) + y).astype(BF16)
        return c
    for p in range(parts):
        x_copy(p).wait()
        lax.fori_loop(p * part // block, (p + 1) * part // block, step, 0)
        out_copy(p).start()
    for p in range(parts):
        out_copy(p).wait()


def spec(space):
    return pl.BlockSpec(memory_space=space)


SMEM = pltpu.SMEM
VMEM = pltpu.VMEM
ANY = pl.ANY


def params(number=None):
    if number is None:
        return pltpu.CompilerParams(vmem_limit_bytes=VMEM_LIMIT)
    return pltpu.CompilerParams(vmem_limit_bytes=VMEM_LIMIT, collective_id=number, has_side_effects=True)


def solution(mesh):
    devs = mesh.shape['ep']
    row_spec = P(('dp', 'ep'), None)
    expert_spec = P('ep', None, None)
    classes = [[i for i in range(devs) if i % CORES == c] for c in range(CORES)]
    partner = [(i, i ^ 1) for i in range(devs)]
    dma = pltpu.SemaphoreType.DMA

    def local_step(x_rows, logits, w_in, w_out):
        tokens, d_model = x_rows.shape
        experts = logits.shape[1]
        exp_dev, _, hidden = w_in.shape
        capacity = CAP_FACTOR * tokens * devs // experts
        cap_slot = capslot(tokens, experts)
        exp_chip = CORES * exp_dev
        chips = devs // CORES
        half = chips // 2
        full = exp_chip * cap_slot
        sizes = tuple(full * k // 64 for k in (43, 48, 64))
        core = (lax.axis_index('ep').astype(I32) % CORES).reshape(1)

        row, keep, start, cnt, back_map, pick = pl.pallas_call(
            functools.partial(route_kernel, sizes, capacity, exp_dev), name='route',
            out_shape=(jax.ShapeDtypeStruct((8, tokens), I32), jax.ShapeDtypeStruct((8, tokens), F32),
                       jax.ShapeDtypeStruct((exp_chip, chips), I32), jax.ShapeDtypeStruct((exp_chip, chips), I32),
                       jax.ShapeDtypeStruct((chips, full), I32), jax.ShapeDtypeStruct((8, LANE), I32)),
            in_specs=[spec(VMEM)],
            scratch_shapes=[VMEM((8, experts), F32), VMEM((devs, 8, experts), F32), dma((devs,)), dma((devs,))],
            compiler_params=params(0))(logits)

        def pack(size, row, x_rows):
            return pl.pallas_call(
                functools.partial(send_kernel, size), name='send',
                out_shape=jax.ShapeDtypeStruct((chips, size, SUB, LANE), BF16),
                in_specs=[spec(SMEM), spec(ANY)], out_specs=spec(ANY),
                scratch_shapes=[SMEM((chips * size + 8,), I32), VMEM((tokens, d_model), BF16),
                                VMEM((tokens, SUB, LANE), BF16), VMEM((4, size, SUB, LANE), BF16),
                                dma((4,)), dma((4,))],
                compiler_params=params())(row, x_rows)

        def combine(size, row, keep, x_rows, back):
            return pl.pallas_call(
                combine_kernel, name='combine', out_shape=jax.ShapeDtypeStruct((tokens, d_model), BF16),
                in_specs=[spec(SMEM)] * 2 + [spec(ANY)] * 2, out_specs=spec(ANY),
                scratch_shapes=[VMEM((chips * size, SUB, LANE), BF16), VMEM((tokens, d_model), BF16),
                                VMEM((tokens, d_model), BF16), VMEM((16, SUB, LANE), F32),
                                dma((chips,)), dma((4,)), dma((4,))],
                compiler_params=params())(row, keep, x_rows, back)

        def fused(number, size, x_rows, w_in, w_out, row, keep, start, cnt, back_map):
            lane_shape = jax.ShapeDtypeStruct((chips, size, SUB, LANE), BF16)
            send = pack(size, row, x_rows)
            back, _, _ = pl.pallas_call(
                functools.partial(moe_kernel, size, cap_slot), name='moe',
                out_shape=(lane_shape, jax.ShapeDtypeStruct(w_in.shape, BF16),
                           jax.ShapeDtypeStruct(w_out.shape, BF16)),
                in_specs=[spec(SMEM)] * 2 + [spec(ANY)] * 3, out_specs=(spec(ANY),) * 3,
                scratch_shapes=[
                    VMEM((half * size + cap_slot, SUB, LANE), BF16),
                    VMEM((half * size + cap_slot, SUB, LANE), BF16),
                    VMEM((chips, size, SUB, LANE), BF16),
                    VMEM((exp_chip * half * cap_slot, SUB, LANE), BF16),
                    VMEM((WEIGHT_SLOTS, d_model, hidden), BF16), VMEM((WEIGHT_SLOTS, hidden, d_model), BF16),
                    VMEM((half * cap_slot, d_model), BF16),
                    dma((chips,)), dma((chips,)), dma((chips,)), dma((chips,)),
                    dma((2, exp_dev)), dma((2, exp_dev)), dma((2, WEIGHT_SLOTS))],
                compiler_params=params(number))(start, back_map, send, w_in, w_out)
            return combine(size, row, keep, x_rows, back)

        def general(size, x_rows, w_in, w_out, row, keep, start, cnt, back_map):
            w_in_p = lax.ppermute(w_in, 'ep', partner)
            w_out_p = lax.ppermute(w_out, 'ep', partner)
            send = pack(size, row, x_rows)
            recv = lax.all_to_all(send, 'ep', 0, 0, axis_index_groups=classes, tiled=True)
            rows_max = capacity + cap_slot
            ret = pl.pallas_call(
                functools.partial(ffn_kernel, size, cap_slot), name='ffn',
                out_shape=jax.ShapeDtypeStruct((chips, size, SUB, LANE), BF16),
                in_specs=[spec(SMEM)] * 3 + [spec(ANY)] * 5, out_specs=spec(ANY),
                scratch_shapes=[
                    VMEM((chips * size + cap_slot, SUB, LANE), BF16),
                    VMEM((chips, size + cap_slot, SUB, LANE), BF16),
                    VMEM((2, d_model, hidden), BF16), VMEM((2, hidden, d_model), BF16),
                    VMEM((rows_max, SUB, LANE), BF16), VMEM((rows_max, SUB, LANE), BF16),
                    VMEM((LANE, d_model), BF16), dma((chips,)), dma((2, 2)), dma((chips,))],
                compiler_params=params())(start, cnt, core, recv, w_in, w_in_p, w_out, w_out_p)
            back = lax.all_to_all(ret, 'ep', 0, 0, axis_index_groups=classes, tiled=True)
            return combine(size, row, keep, x_rows, back)

        branches = [functools.partial(fused, 1 + k, size) for k, size in enumerate(sizes[:-1])]
        branches.append(functools.partial(general, sizes[-1]))
        return lax.switch(pick[0, 0], branches, x_rows, w_in, w_out, row, keep, start, cnt, back_map)

    return jax.shard_map(local_step, mesh=mesh, in_specs=(row_spec, row_spec, expert_spec, expert_spec),
                         out_specs=row_spec, check_vma=False)
```

```python
import functools

import jax
import jax.numpy as jnp
from jax import lax
from jax.experimental import pallas as pl
from jax.experimental.pallas import tpu as pltpu
from jax.sharding import PartitionSpec as P

CAP_FACTOR = 2
SLOT_FACTOR = 4
CORES = 2
SUB = 16
WEIGHT_SLOTS = 6
LANE = 128
VMEM_LIMIT = 62 * 1024 * 1024
BF16 = jnp.bfloat16
F32 = jnp.float32
I32 = jnp.int32


MESH = pl.DeviceIdType.MESH


def iota(shape, dim):
    return lax.broadcasted_iota(I32, shape, dim)


def route_kernel(sizes, capacity, exp_dev, logits_ref, row_ref, keep_ref, start_ref, cnt_ref, back_ref, pick_ref,
                 stage, counts_v, send_sem, recv_sem):
    tokens, experts = logits_ref.shape
    devs = counts_v.shape[0]
    exp_chip = CORES * exp_dev
    me = lax.axis_index('ep')
    chip = me // CORES
    core = me % CORES
    barrier = pltpu.get_barrier_semaphore()

    def other(d):
        return {'ep': (me + d) % devs}

    def hello(d, c):
        pl.semaphore_signal(barrier, inc=1, device_id=other(d), device_id_type=MESH)
        return c
    lax.fori_loop(1, devs, hello, 0)

    lt = logits_ref[...].T
    ids = iota(lt.shape, 0)
    m1 = jnp.max(lt, axis=0, keepdims=True)
    e1 = jnp.min(jnp.where(lt == m1, ids, experts), axis=0, keepdims=True)
    rest = jnp.where(ids == e1, -jnp.inf, lt)
    m2 = jnp.max(rest, axis=0, keepdims=True)
    e2 = jnp.min(jnp.where(rest == m2, ids, experts), axis=0, keepdims=True)
    hit1 = ids == e1
    hit2 = ids == e2
    chosen = jnp.where(hit1 | hit2, 1.0, 0.0).astype(BF16)
    ones = jnp.ones((8, tokens), BF16)
    count = lax.dot_general(ones, chosen, (((1,), (1,)), ((), ())), preferred_element_type=F32)
    stage[...] = count
    counts_v[me] = count
    pl.semaphore_wait(barrier, devs - 1)

    def copy(d):
        return pltpu.make_async_remote_copy(
            src_ref=stage, dst_ref=counts_v.at[me], send_sem=send_sem.at[d], recv_sem=recv_sem.at[d],
            device_id=other(d), device_id_type=MESH)

    def start_copy(d, c):
        copy(d).start()
        return c

    total = jnp.sum(jnp.exp(lt - m1), axis=0, keepdims=True)
    gates = (1.0 / total, jnp.exp(m2 - m1) / total)
    lax.fori_loop(1, devs, start_copy, 0)
    upper = jnp.where(iota((tokens, tokens), 0) < iota((tokens, tokens), 1), 1.0, 0.0).astype(BF16)
    before = jnp.dot(chosen, upper, preferred_element_type=F32)
    pos1 = jnp.sum(jnp.where(hit1, before, 0.0), axis=0, keepdims=True).astype(I32)
    pos2 = jnp.sum(jnp.where(hit2, before, 0.0), axis=0, keepdims=True).astype(I32)

    def wait_copy(d, c):
        copy(d).wait()
        return c
    lax.fori_loop(1, devs, wait_copy, 0)

    counts = counts_v[:, 0, :]
    lower = jnp.where(iota((devs, devs), 1) < iota((devs, devs), 0), 1.0, 0.0).astype(BF16)
    offs = jnp.dot(lower, counts.astype(BF16), preferred_element_type=F32)
    kept = jnp.minimum(jnp.maximum(capacity - offs, 0.0), counts)
    kept_b = kept.astype(BF16)
    row_e = iota((experts, experts), 0)
    col_e = iota((experts, experts), 1)
    same = (row_e // exp_chip == col_e // exp_chip) & (row_e < col_e)
    start = jnp.dot(kept_b, jnp.where(same, 1.0, 0.0).astype(BF16), preferred_element_type=F32)
    start_b = start.astype(BF16)
    member = jnp.where(iota((experts, LANE), 0) // exp_chip == iota((experts, LANE), 1), 1.0, 0.0).astype(BF16)
    totals = jnp.dot(kept_b, member, preferred_element_type=F32)
    most = jnp.max(jnp.max(totals, axis=0, keepdims=True), axis=1, keepdims=True).astype(I32)
    size = jnp.full((1, 1), sizes[0], I32)
    pick = jnp.zeros((1, 1), I32)
    for small, large in zip(sizes[:-1], sizes[1:]):
        size = jnp.where(most > small, large, size)
        pick = pick + jnp.where(most > small, 1, 0)
    pick_ref[...] = jnp.broadcast_to(pick, pick_ref.shape)

    mine = iota((devs, experts), 0) == me
    my_start = jnp.sum(jnp.where(mine, start, 0.0), axis=0, keepdims=True)
    my_kept = jnp.sum(jnp.where(mine, kept, 0.0), axis=0, keepdims=True)
    look = jnp.concatenate([my_start, my_kept, jnp.zeros((6, experts), F32)], axis=0).astype(BF16)
    lanes = experts // exp_chip
    for k, (e, hit, pos) in enumerate(((e1, hit1, pos1), (e2, hit2, pos2))):
        got = jnp.dot(look, jnp.where(hit, 1.0, 0.0).astype(BF16), preferred_element_type=F32).astype(I32)
        keep = pos < got[1:2, :]
        row = (e // exp_chip) * size + got[0:1, :] + pos
        row_ref[k:k + 1, :] = jnp.where(keep, row, lanes * size)
        keep_ref[k:k + 1, :] = jnp.where(keep, gates[k], 0.0)

    srcs = devs // CORES
    pick_src = jnp.where(iota((srcs, devs), 1) == CORES * iota((srcs, devs), 0) + core, 1.0, 0.0).astype(BF16)
    pick_exp = jnp.where(iota((exp_chip, experts), 1) == chip * exp_chip + iota((exp_chip, experts), 0),
                         1.0, 0.0).astype(BF16)
    contract = (((1,), (1,)), ((), ()))

    def mine_of(table):
        part = lax.dot_general(pick_exp, table, contract, preferred_element_type=F32).astype(BF16)
        return lax.dot_general(part, pick_src, contract, preferred_element_type=F32).astype(I32)
    first = mine_of(start_b)
    count = mine_of(kept_b)
    start_ref[...] = first
    cnt_ref[...] = count
    width = back_ref.shape[1]
    ids = iota((exp_chip, width), 0)
    rows = iota((exp_chip, width), 1)
    group_rows = (srcs // 2) * capslot(tokens, experts)
    for s in range(srcs):
        off = rows - first[:, s:s + 1]
        inside = (off >= 0) & (off < count[:, s:s + 1])
        back_ref[s:s + 1, :] = jnp.sum(jnp.where(inside, ids * group_rows + off, 0), axis=0, keepdims=True)


def unroll(size):
    return max(k for k in range(1, 49) if size % k == 0)


def send_kernel(size, row_ref, x_ref, out_ref, tok, x_v, rows3, stage, x_sem, sem):
    tokens, d_model = x_ref.shape
    lanes = out_ref.shape[0]
    block = 16
    parts = x_sem.shape[0]
    part = tokens // parts

    def x_copy(p):
        rows = pl.ds(p * part, part)
        return pltpu.make_async_copy(x_ref.at[rows], x_v.at[rows], x_sem.at[p])
    for p in range(parts):
        x_copy(p).start()

    def relayout(i, c):
        r = pl.ds(pl.multiple_of(i * block, block), block)
        rows3[r] = x_v[r].astype(F32).reshape(block, SUB, LANE).astype(BF16)
        for u in range(block):
            t = i * block + u
            tok[row_ref[0, t]] = t
            tok[row_ref[1, t]] = t
        return c
    for p in range(parts):
        x_copy(p).wait()
        lax.fori_loop(p * part // block, (p + 1) * part // block, relayout, 0)

    slots = stage.shape[0]
    step = unroll(size)

    def copy(lane, slot):
        return pltpu.make_async_copy(stage.at[slot], out_ref.at[lane], sem.at[slot])

    def lane_step(lane, c):
        slot = lane % slots

        @pl.when(lane >= slots)
        def _():
            copy(lane - slots, slot).wait()

        def rows(i, c2):
            for u in range(step):
                r = i * step + u
                t = tok[lane * size + r]
                t = t & (tokens - 1) if tokens & (tokens - 1) == 0 else jnp.clip(t, 0, tokens - 1)
                stage[slot, r] = rows3[t]
            return c2
        lax.fori_loop(0, size // step, rows, 0)
        copy(lane, slot).start()
        return c
    lax.fori_loop(0, lanes, lane_step, 0)
    for k in range(min(slots, lanes)):
        lane = lanes - min(slots, lanes) + k
        copy(lane, lane % slots).wait()


def capslot(tokens, experts):
    return SLOT_FACTOR * tokens // experts


def grid_side(chips):
    return max(k for k in range(1, chips + 1) if chips % k == 0 and k * k <= chips)


def shifts_of(chips):
    side = grid_side(chips)
    tall = chips // side
    steps = [(dy, dx) for dy in range(tall) for dx in range(side)]
    near = [s for s in steps if s != (0, 0) and 2 * s[0] != tall and 2 * s[1] != side]
    if 2 * len(near) != chips:
        near = [s for s in steps if (s[0] + s[1]) % 2 == 0]
    far = [s for s in steps if s not in near]
    turn = (tall - 1) * (side - 1) + 1

    def rank(s):
        return (0 in s, s == (0, 0), s[1] == 0, (s[0] * turn + s[1]) % 2, s[0] != s[1])
    return sorted(near, key=rank), sorted(far, key=rank)


def moe_kernel(size, cap_slot, start_ref, map_ref, send_ref, w1o, w2o, back_ref, w1p, w2p,
               recv_a, recv_b, ret_v, ze, w1_v, w2_v, x2,
               out_sem, in_sem, ret_out_sem, ret_in_sem, swap_out_sem, swap_in_sem, w_sem):
    chips = send_ref.shape[0]
    exp_dev = w1o.shape[0]
    exp_chip = CORES * exp_dev
    groups = shifts_of(chips)
    half = len(groups[0])
    side = grid_side(chips)
    tall = chips // side
    me = lax.axis_index('ep')
    chip = me // CORES
    core = me % CORES
    cy = chip // side
    cx = chip % side
    partner = {'ep': chip * CORES + (1 - core)}

    def ahead(step):
        return ((cy + step[0]) % tall) * side + (cx + step[1]) % side

    def behind(step):
        return ((cy + tall - step[0]) % tall) * side + (cx + side - step[1]) % side

    def device(c):
        return {'ep': c * CORES + core}

    barrier = pltpu.get_barrier_semaphore()
    pl.semaphore_signal(barrier, inc=1, device_id=partner, device_id_type=MESH)
    for step in groups[0] + groups[1]:
        if step != (0, 0):
            pl.semaphore_signal(barrier, inc=1, device_id=device(ahead(step)), device_id_type=MESH)
    pl.semaphore_wait(barrier, chips)

    recvs = (recv_a, recv_b)

    def dispatch(g, q):
        step = groups[g][q]
        n = g * half + q
        dst = recvs[g].at[pl.ds(q * size, size)]
        if step == (0, 0):
            return pltpu.make_async_copy(send_ref.at[chip], dst, in_sem.at[n])
        to = ahead(step)
        return pltpu.make_async_remote_copy(
            src_ref=send_ref.at[to], dst_ref=dst, send_sem=out_sem.at[n], recv_sem=in_sem.at[n],
            device_id=device(to), device_id_type=MESH)

    def swap(k, j):
        src, dst = ((w1o, w1p), (w2o, w2p))[k]
        return pltpu.make_async_remote_copy(
            src_ref=src.at[j], dst_ref=dst.at[j], send_sem=swap_out_sem.at[k, j], recv_sem=swap_in_sem.at[k, j],
            device_id=partner, device_id_type=MESH)

    def give(g, q):
        step = groups[g][q]
        n = g * half + q
        src = ret_v.at[n]
        if step == (0, 0):
            return pltpu.make_async_copy(src, back_ref.at[chip], ret_in_sem.at[n])
        return pltpu.make_async_remote_copy(
            src_ref=src, dst_ref=back_ref.at[chip], send_sem=ret_out_sem.at[n], recv_sem=ret_in_sem.at[n],
            device_id=device(behind(step)), device_id_type=MESH)

    def dispatch_start(g, late):
        for q in range(half):
            if (groups[g][q][1] == 0) == late:
                dispatch(g, q).start()

    def dispatch_end(g, q):
        if groups[g][q] == (0, 0):
            dispatch(g, q).wait()
        else:
            dispatch(g, q).wait_recv()

    dispatch_start(0, False)

    def swap_start(j, c):
        swap(0, j).start()
        swap(1, j).start()
        return c
    lax.fori_loop(0, exp_dev, swap_start, 0)

    slots = w1_v.shape[0]

    def load(a, b, j, slot):
        return (pltpu.make_async_copy(a.at[j], w1_v.at[slot], w_sem.at[0, slot]),
                pltpu.make_async_copy(b.at[j], w2_v.at[slot], w_sem.at[1, slot]))

    def load_start(p, slot, first):
        @pl.when(p < exp_dev)
        def _():
            for d in load(w1o, w2o, p, slot):
                d.start()

        @pl.when(p >= exp_dev)
        def _():
            j = p - exp_dev
            if first:
                swap(0, j).wait_recv()
                swap(1, j).wait_recv()
            for d in load(w1p, w2p, j, slot):
                d.start()

    def load_wait(slot):
        for d in load(w1o, w2o, 0, slot):
            d.wait()

    def compute(g, i, slot):
        recv = recvs[g]
        for q in range(half):
            a = start_ref[i, behind(groups[g][q])] + q * size
            v = jnp.stack([recv[a + j] for j in range(cap_slot)]).astype(F32)
            x2[pl.ds(q * cap_slot, cap_slot), :] = v.reshape(cap_slot, SUB * LANE).astype(BF16)
        h = jnp.dot(x2[...], w1_v[slot], preferred_element_type=F32)
        h = jax.nn.gelu(h, approximate=True).astype(BF16)
        z = jnp.dot(h, w2_v[slot], preferred_element_type=F32).astype(BF16).astype(F32)
        rows = half * cap_slot
        ze[pl.ds(pl.multiple_of(i * rows, rows), rows)] = z.reshape(rows, SUB, LANE).astype(BF16)

    def is_late(g, q):
        return groups[g][q][1] == 0

    def pack_back(g):
        for q in range(half):
            lane = behind(groups[g][q])
            n = g * half + q

            def rows(b, c):
                for u in range(unroll(size)):
                    r = b * unroll(size) + u
                    ret_v[n, r] = ze[map_ref[lane, r] + q * cap_slot]
                return c
            lax.fori_loop(0, size // unroll(size), rows, 0)
            if q > 0 and not is_late(g, q - 1):
                give(g, q - 1).start()
        if not is_late(g, half - 1):
            give(g, half - 1).start()

    def give_late(g):
        for q in range(half):
            if is_late(g, q):
                give(g, q).start()

    depth = slots - 1
    for p in range(depth):
        for d in load(w1o, w2o, p, p):
            d.start()
    early = [q for q in range(half) if not is_late(0, q)]
    late = [q for q in range(half) if is_late(0, q)]
    for q in early[:half // 2]:
        dispatch_end(0, q)
    dispatch_start(0, True)
    dispatch_start(1, False)
    for q in early[half // 2:] + late:
        dispatch_end(0, q)

    def first_pass(p, c):
        @pl.when(p + depth < exp_chip)
        def _():
            load_start(p + depth, (p + depth) % slots, True)

        @pl.when(p == exp_dev)
        def _():
            dispatch_start(1, True)
        slot = p % slots
        load_wait(slot)
        compute(0, (core * exp_dev + p) % exp_chip, slot)
        return c
    lax.fori_loop(0, exp_chip, first_pass, 0)
    pack_back(0)
    for q in range(half):
        dispatch_end(1, q)
    give_late(0)
    held = exp_chip - slots

    def second_pass(b, c):
        slot = (held + b) % slots

        @pl.when(b >= slots)
        def _():
            load_wait(slot)
        compute(1, (core * exp_dev + held + b) % exp_chip, slot)

        @pl.when(b < held)
        def _():
            load_start(b, slot, False)
        return c
    lax.fori_loop(0, exp_chip, second_pass, 0)
    pack_back(1)
    for q in range(half):
        give(0, q).wait_recv() if groups[0][q] != (0, 0) else give(0, q).wait()
    give_late(1)

    def swap_end(j, c):
        swap(0, j).wait_send()
        swap(1, j).wait_send()
        return c
    lax.fori_loop(0, exp_dev, swap_end, 0)
    for g in range(2):
        for q in range(half):
            if groups[g][q] != (0, 0):
                dispatch(g, q).wait_send()
                give(g, q).wait_send()
            if g == 1:
                give(g, q).wait() if groups[g][q] == (0, 0) else give(g, q).wait_recv()


def ffn_kernel(size, cap_slot, start_ref, cnt_ref, core_ref, recv_ref, w1o, w1p, w2o, w2p, out_ref,
               recv_v, ret_v, w1_v, w2_v, xe, ze, x2, recv_sem, w_sem, out_sem):
    srcs = recv_ref.shape[0]
    exp_dev = w1o.shape[0]
    exp_chip = CORES * exp_dev
    core = core_ref[0]
    block = x2.shape[0]

    def recv_copy(s):
        return pltpu.make_async_copy(recv_ref.at[s], recv_v.at[pl.ds(s * size, size)], recv_sem.at[s])

    def out_copy(s):
        return pltpu.make_async_copy(ret_v.at[s, pl.ds(0, size)], out_ref.at[s], out_sem.at[s])

    def w_start(i):
        slot = i % 2
        local = i % exp_dev

        @pl.when(i // exp_dev == core)
        def _():
            pltpu.make_async_copy(w1o.at[local], w1_v.at[slot], w_sem.at[0, slot]).start()
            pltpu.make_async_copy(w2o.at[local], w2_v.at[slot], w_sem.at[1, slot]).start()

        @pl.when(i // exp_dev != core)
        def _():
            pltpu.make_async_copy(w1p.at[local], w1_v.at[slot], w_sem.at[0, slot]).start()
            pltpu.make_async_copy(w2p.at[local], w2_v.at[slot], w_sem.at[1, slot]).start()

    def w_wait(i):
        slot = i % 2
        pltpu.make_async_copy(w1o.at[0], w1_v.at[slot], w_sem.at[0, slot]).wait()
        pltpu.make_async_copy(w2o.at[0], w2_v.at[slot], w_sem.at[1, slot]).wait()

    for s in range(srcs):
        recv_copy(s).start()
    w_start(jnp.int32(0))
    for s in range(srcs):
        recv_copy(s).wait()

    def expert(i, c):
        slot = i % 2

        @pl.when(i + 1 < exp_chip)
        def _():
            w_start(i + 1)

        def gather(s, pos):
            n = cnt_ref[i, s]

            @pl.when(n > 0)
            def _():
                a = s * size + start_ref[i, s]
                for j in range(cap_slot):
                    xe[pos + j] = recv_v[a + j]
            return pos + n
        total = lax.fori_loop(0, srcs, gather, jnp.int32(0))
        w_wait(i)

        def tile(b, c2):
            base = pl.multiple_of(b * block, block)
            for q in range(block // 16):
                v = xe[pl.ds(base + q * 16, 16)].astype(F32).reshape(16, SUB * LANE)
                x2[pl.ds(q * 16, 16), :] = v.astype(BF16)
            h = jnp.dot(x2[...], w1_v[slot], preferred_element_type=F32)
            h = jax.nn.gelu(h, approximate=True).astype(BF16)
            z = jnp.dot(h, w2_v[slot], preferred_element_type=F32).astype(BF16).astype(F32)
            ze[pl.ds(base, block)] = z.reshape(block, SUB, LANE).astype(BF16)
            return c2
        lax.fori_loop(0, (total + block - 1) // block, tile, 0)

        def scatter(s, pos):
            n = cnt_ref[i, s]

            @pl.when(n > 0)
            def _():
                a = start_ref[i, s]
                for j in range(cap_slot):
                    ret_v[s, a + j] = ze[pos + j]
            return pos + n
        lax.fori_loop(0, srcs, scatter, jnp.int32(0))
        return c
    lax.fori_loop(0, exp_chip, expert, 0)
    for s in range(srcs):
        out_copy(s).start()
    for s in range(srcs):
        out_copy(s).wait()


def combine_kernel(row_ref, gate_ref, x_ref, ret_ref, out_ref, ret_v, x_v, out_v, y3, sem, x_sem, out_sem):
    tokens, d_model = x_ref.shape
    lanes, size = ret_ref.shape[:2]
    last = lanes * size - 1
    block = 16
    parts = x_sem.shape[0]
    part = tokens // parts

    def copy(s):
        return pltpu.make_async_copy(ret_ref.at[s], ret_v.at[pl.ds(s * size, size)], sem.at[s])

    def x_copy(p):
        rows = pl.ds(p * part, part)
        return pltpu.make_async_copy(x_ref.at[rows], x_v.at[rows], x_sem.at[p])

    def out_copy(p):
        rows = pl.ds(p * part, part)
        return pltpu.make_async_copy(out_v.at[rows], out_ref.at[rows], out_sem.at[p])
    for s in range(lanes):
        copy(s).start()
    for p in range(parts):
        x_copy(p).start()
    for s in range(lanes):
        copy(s).wait()

    def step(i, c):
        base = pl.multiple_of(i * block, block)
        for u in range(block):
            t = base + u
            g1 = gate_ref[0, t]
            g2 = gate_ref[1, t]
            z1 = ret_v[jnp.minimum(row_ref[0, t], last)].astype(F32)
            z2 = ret_v[jnp.minimum(row_ref[1, t], last)].astype(F32)
            y3[u] = jnp.where(g1 > 0, g1 * z1, 0.0) + jnp.where(g2 > 0, g2 * z2, 0.0)
        r = pl.ds(base, block)
        y = y3[...].reshape(block, d_model)
        out_v[r, :] = (x_v[r, :].astype(F32) + y).astype(BF16)
        return c
    for p in range(parts):
        x_copy(p).wait()
        lax.fori_loop(p * part // block, (p + 1) * part // block, step, 0)
        out_copy(p).start()
    for p in range(parts):
        out_copy(p).wait()


def spec(space):
    return pl.BlockSpec(memory_space=space)


SMEM = pltpu.SMEM
VMEM = pltpu.VMEM
ANY = pl.ANY


def params(number=None):
    if number is None:
        return pltpu.CompilerParams(vmem_limit_bytes=VMEM_LIMIT)
    return pltpu.CompilerParams(vmem_limit_bytes=VMEM_LIMIT, collective_id=number, has_side_effects=True)


def solution(mesh):
    devs = mesh.shape['ep']
    row_spec = P(('dp', 'ep'), None)
    expert_spec = P('ep', None, None)
    classes = [[i for i in range(devs) if i % CORES == c] for c in range(CORES)]
    partner = [(i, i ^ 1) for i in range(devs)]
    dma = pltpu.SemaphoreType.DMA

    def local_step(x_rows, logits, w_in, w_out):
        tokens, d_model = x_rows.shape
        experts = logits.shape[1]
        exp_dev, _, hidden = w_in.shape
        capacity = CAP_FACTOR * tokens * devs // experts
        cap_slot = capslot(tokens, experts)
        exp_chip = CORES * exp_dev
        chips = devs // CORES
        half = chips // 2
        full = exp_chip * cap_slot
        sizes = tuple(full * k // 64 for k in (42, 46, 64))
        core = (lax.axis_index('ep').astype(I32) % CORES).reshape(1)

        row, keep, start, cnt, back_map, pick = pl.pallas_call(
            functools.partial(route_kernel, sizes, capacity, exp_dev), name='route',
            out_shape=(jax.ShapeDtypeStruct((8, tokens), I32), jax.ShapeDtypeStruct((8, tokens), F32),
                       jax.ShapeDtypeStruct((exp_chip, chips), I32), jax.ShapeDtypeStruct((exp_chip, chips), I32),
                       jax.ShapeDtypeStruct((chips, full), I32), jax.ShapeDtypeStruct((8, LANE), I32)),
            in_specs=[spec(VMEM)],
            scratch_shapes=[VMEM((8, experts), F32), VMEM((devs, 8, experts), F32), dma((devs,)), dma((devs,))],
            compiler_params=params(0))(logits)

        def pack(size, row, x_rows):
            return pl.pallas_call(
                functools.partial(send_kernel, size), name='send',
                out_shape=jax.ShapeDtypeStruct((chips, size, SUB, LANE), BF16),
                in_specs=[spec(SMEM), spec(ANY)], out_specs=spec(ANY),
                scratch_shapes=[SMEM((chips * size + 8,), I32), VMEM((tokens, d_model), BF16),
                                VMEM((tokens, SUB, LANE), BF16), VMEM((4, size, SUB, LANE), BF16),
                                dma((4,)), dma((4,))],
                compiler_params=params())(row, x_rows)

        def combine(size, row, keep, x_rows, back):
            return pl.pallas_call(
                combine_kernel, name='combine', out_shape=jax.ShapeDtypeStruct((tokens, d_model), BF16),
                in_specs=[spec(SMEM)] * 2 + [spec(ANY)] * 2, out_specs=spec(ANY),
                scratch_shapes=[VMEM((chips * size, SUB, LANE), BF16), VMEM((tokens, d_model), BF16),
                                VMEM((tokens, d_model), BF16), VMEM((16, SUB, LANE), F32),
                                dma((chips,)), dma((4,)), dma((4,))],
                compiler_params=params())(row, keep, x_rows, back)

        def fused(number, size, x_rows, w_in, w_out, row, keep, start, cnt, back_map):
            lane_shape = jax.ShapeDtypeStruct((chips, size, SUB, LANE), BF16)
            send = pack(size, row, x_rows)
            back, _, _ = pl.pallas_call(
                functools.partial(moe_kernel, size, cap_slot), name='moe',
                out_shape=(lane_shape, jax.ShapeDtypeStruct(w_in.shape, BF16),
                           jax.ShapeDtypeStruct(w_out.shape, BF16)),
                in_specs=[spec(SMEM)] * 2 + [spec(ANY)] * 3, out_specs=(spec(ANY),) * 3,
                scratch_shapes=[
                    VMEM((half * size + cap_slot, SUB, LANE), BF16),
                    VMEM((half * size + cap_slot, SUB, LANE), BF16),
                    VMEM((chips, size, SUB, LANE), BF16),
                    VMEM((exp_chip * half * cap_slot, SUB, LANE), BF16),
                    VMEM((WEIGHT_SLOTS, d_model, hidden), BF16), VMEM((WEIGHT_SLOTS, hidden, d_model), BF16),
                    VMEM((half * cap_slot, d_model), BF16),
                    dma((chips,)), dma((chips,)), dma((chips,)), dma((chips,)),
                    dma((2, exp_dev)), dma((2, exp_dev)), dma((2, WEIGHT_SLOTS))],
                compiler_params=params(number))(start, back_map, send, w_in, w_out)
            return combine(size, row, keep, x_rows, back)

        def general(size, x_rows, w_in, w_out, row, keep, start, cnt, back_map):
            w_in_p = lax.ppermute(w_in, 'ep', partner)
            w_out_p = lax.ppermute(w_out, 'ep', partner)
            send = pack(size, row, x_rows)
            recv = lax.all_to_all(send, 'ep', 0, 0, axis_index_groups=classes, tiled=True)
            rows_max = capacity + cap_slot
            ret = pl.pallas_call(
                functools.partial(ffn_kernel, size, cap_slot), name='ffn',
                out_shape=jax.ShapeDtypeStruct((chips, size, SUB, LANE), BF16),
                in_specs=[spec(SMEM)] * 3 + [spec(ANY)] * 5, out_specs=spec(ANY),
                scratch_shapes=[
                    VMEM((chips * size + cap_slot, SUB, LANE), BF16),
                    VMEM((chips, size + cap_slot, SUB, LANE), BF16),
                    VMEM((2, d_model, hidden), BF16), VMEM((2, hidden, d_model), BF16),
                    VMEM((rows_max, SUB, LANE), BF16), VMEM((rows_max, SUB, LANE), BF16),
                    VMEM((LANE, d_model), BF16), dma((chips,)), dma((2, 2)), dma((chips,))],
                compiler_params=params())(start, cnt, core, recv, w_in, w_in_p, w_out, w_out_p)
            back = lax.all_to_all(ret, 'ep', 0, 0, axis_index_groups=classes, tiled=True)
            return combine(size, row, keep, x_rows, back)

        branches = [functools.partial(fused, 1 + k, size) for k, size in enumerate(sizes[:-1])]
        branches.append(functools.partial(general, sizes[-1]))
        return lax.switch(pick[0, 0], branches, x_rows, w_in, w_out, row, keep, start, cnt, back_map)

    return jax.shard_map(local_step, mesh=mesh, in_specs=(row_spec, row_spec, expert_spec, expert_spec),
                         out_specs=row_spec, check_vma=False)
```
